16 devices in a mesh: dp: 4 (over z, y), stage: 4 (over x, core).
Axes of the slice: x: 2, y: 2, z: 2, core: 2. Of those that a mesh axis runs over, the one named last changes fastest.
Arguments:
- token_ids: int32 [32, 256], P('dp'), parts along dimension 0
- label_ids: int32 [32, 256], P('dp'), parts along dimension 0
- embedding: bfloat16 [49152, 960], P('stage')
- w_in: bfloat16 [4, 960, 2560], P('stage')
- w_out: bfloat16 [4, 2560, 960], P('stage')
Outputs:
- output 1: float32 [4], P('dp'), parts along dimension 0
- output 2: float32 [16, 960, 2560], P(('dp', 'stage')), parts along dimension 0
- output 3: float32 [16, 2560, 960], P(('dp', 'stage')), parts along dimension 0
- output 4: float32 [196608, 960], P(('dp', 'stage')), parts along dimension 0
There are 4 independent parts. The reference program is written for one: setup_inputs(seed, part) draws one part's arguments, and reference() takes and returns one part's arrays. A program takes and returns all parts, laid end to end along the dimension named above; an argument that names none is the same for every part.
All inputs are finite; a program needn't handle non-finite values.
Results may differ from the reference program's by a relative error of at most 0.0110023.
Values are sent between devices in bfloat16 or wider.
A program may use at most 1 GiB of HBM per device.

```python
import functools
import jax
import jax.numpy as jnp
from jax import lax

VOCAB_SIZE = 49152
MODEL_DIM = 960
FFN_DIM = 2560
STAGES = 4
MICROBATCHES = 8
MICRO_TOKENS = 256
HOT_IDS = 64
NORM_EPS = 1e-6


def draw_ids(hot_ids, id_key):
    key_pick, key_unif, key_mix = jax.random.split(id_key, 3)
    shape_ids = (MICROBATCHES, MICRO_TOKENS)
    picked = hot_ids[jax.random.randint(key_pick, shape_ids, 0, HOT_IDS)]
    uniform_ids = jax.random.randint(key_unif, shape_ids, 0, VOCAB_SIZE)
    use_hot = jax.random.randint(key_mix, shape_ids, 0, 2) == 1
    return jnp.where(use_hot, picked, uniform_ids).astype(jnp.int32)


def setup_inputs(seed: int = 0, part: int = 0) -> dict:
    root_key = jax.random.key(seed)
    key_ids, key_emb, key_in, key_out = jax.random.split(root_key, 4)
    part_key = jax.random.fold_in(key_ids, part)
    key_hot, key_tok, key_lab = jax.random.split(part_key, 3)
    hot_ids = jax.random.randint(key_hot, (HOT_IDS,), 0, VOCAB_SIZE)
    token_ids = draw_ids(hot_ids, key_tok)
    label_ids = draw_ids(hot_ids, key_lab)
    embedding = jax.random.normal(key_emb, (VOCAB_SIZE, MODEL_DIM), jnp.float32).astype(jnp.bfloat16)
    w_in = (jax.random.normal(key_in, (STAGES, MODEL_DIM, FFN_DIM), jnp.float32) * MODEL_DIM ** -0.5).astype(jnp.bfloat16)
    w_out = (jax.random.normal(key_out, (STAGES, FFN_DIM, MODEL_DIM), jnp.float32) * 2.0 * (FFN_DIM * STAGES) ** -0.5).astype(jnp.bfloat16)
    return {"token_ids": token_ids, "label_ids": label_ids, "embedding": embedding, "w_in": w_in, "w_out": w_out}


def rms_normed(act_rows):
    acts_f = act_rows.astype(jnp.float32)
    return (acts_f * lax.rsqrt(jnp.mean(acts_f * acts_f, axis=-1, keepdims=True) + NORM_EPS)).astype(jnp.bfloat16)


def summed_loss(emb_f32, w_in_f32, w_out_f32, token_ids, label_ids):
    logit_scale = MODEL_DIM ** -0.5
    vocab_iota = jnp.arange(VOCAB_SIZE, dtype=jnp.int32)

    def layer_step(act_rows, weights):
        w_first, w_second = weights
        acts_f = act_rows.astype(jnp.float32)
        pre_act = jnp.dot(acts_f, w_first, preferred_element_type=jnp.float32)
        hidden = jax.nn.gelu(pre_act).astype(jnp.bfloat16)
        out_f = acts_f + jnp.dot(hidden.astype(jnp.float32), w_second, preferred_element_type=jnp.float32)
        return out_f.astype(jnp.bfloat16), None

    def micro_step(loss_total, ids_pair):
        tok_row, lab_row = ids_pair
        act_rows = emb_f32[tok_row].astype(jnp.bfloat16)
        act_rows, _ = lax.scan(layer_step, act_rows, (w_in_f32, w_out_f32))
        normed = rms_normed(act_rows).astype(jnp.float32)
        logits = jnp.dot(normed, emb_f32.T, preferred_element_type=jnp.float32) * logit_scale
        picked = jnp.sum(jnp.where(lab_row[:, None] == vocab_iota[None, :], logits, 0.0), axis=1)
        return loss_total + jnp.sum(jax.nn.logsumexp(logits, axis=1) - picked), None

    loss_total, _ = lax.scan(jax.checkpoint(micro_step), jnp.zeros((), jnp.float32), (token_ids, label_ids))
    return loss_total


def reference(token_ids, label_ids, embedding, w_in, w_out):
    loss_fn = functools.partial(summed_loss, token_ids=token_ids, label_ids=label_ids)
    loss_total, pull_back = jax.vjp(loss_fn, embedding.astype(jnp.float32), w_in.astype(jnp.float32), w_out.astype(jnp.float32))
    grad_emb, grad_in, grad_out = pull_back(jnp.ones((), jnp.float32))
    mean_loss = (loss_total / (MICROBATCHES * MICRO_TOKENS)).reshape(1)
    return (mean_loss, grad_in, grad_out, grad_emb)
```

```python
import functools

import jax
import jax.numpy as jnp
from jax import lax
from jax.experimental import pallas as pl
from jax.experimental.pallas import tpu as pltpu
from jax.sharding import PartitionSpec as P

NORM_EPS = 1e-6
GELU_A = 0.7978845608028654
GELU_B = 0.044715
NN = (((1,), (0,)), ((), ()))
NT = (((1,), (1,)), ((), ()))
TN = (((0,), (0,)), ((), ()))
MESH = pl.DeviceIdType.MESH
BF16 = jnp.bfloat16
F32 = jnp.float32
VMEM_ALL = 66_000_000
CHUNK = 256
LOOK_TILE = 512
HEAD_ROWS = 512
HEAD_TILE = 1024
FFN_TILE = 512


def mm(lhs, rhs, dims=NN):
    return lax.dot_general(lhs, rhs, dims, preferred_element_type=F32)


def one_hot(match):
    return jnp.where(match, 1.0, 0.0).astype(BF16)


def params(n_axes=0, **kwargs):
    if n_axes:
        kwargs["dimension_semantics"] = ("arbitrary",) * n_axes
    kwargs.setdefault("vmem_limit_bytes", VMEM_ALL)
    return pltpu.CompilerParams(**kwargs)


def vmem():
    return pl.BlockSpec(memory_space=pltpu.VMEM)


def chunk_bounds(starts, tile_idx):
    lo, hi = starts[tile_idx], starts[tile_idx + 1]
    first = lo // CHUNK
    return first, jnp.where(hi > lo, (hi + CHUNK - 1) // CHUNK, first)


def lookup_kernel(starts, ids_ref, rank_ref, table_ref, out_ref, acc, packed):
    tile_idx = pl.program_id(0)
    n_tiles = pl.num_programs(0)
    n_chunk = acc.shape[0]

    @pl.when(tile_idx == 0)
    def _():
        acc[...] = jnp.zeros_like(acc)

    first, last = chunk_bounds(starts, tile_idx)
    base = starts[n_tiles + 1] + tile_idx * LOOK_TILE

    def step(c, _):
        rows = lax.broadcasted_iota(jnp.int32, (LOOK_TILE, CHUNK), 0) + base
        acc[c] += mm(table_ref[...], one_hot(rows == ids_ref[c]))
        return 0

    lax.fori_loop(first, last, step, 0)

    @pl.when(tile_idx == n_tiles - 1)
    def _():
        packed[...] = acc[...].astype(BF16)

        def back(m, _):
            slot = lax.broadcasted_iota(jnp.int32, (rank_ref.shape[1], CHUNK), 1)
            total = mm(one_hot(slot == rank_ref[m]), packed[0], NT)
            for c in range(1, n_chunk):
                total += mm(one_hot(slot + c * CHUNK == rank_ref[m]), packed[c], NT)
            out_ref[m] = total.astype(BF16)
            return 0

        lax.fori_loop(0, out_ref.shape[0], back, 0)


def run_lookup(starts, ids_rows, rank_cols, table_t):
    dim, rows = table_t.shape
    n_micro, tokens = rank_cols.shape[:2]
    n_chunk = n_micro * tokens // CHUNK
    whole = lambda *shape: pl.BlockSpec(shape, lambda i, s: (0,) * len(shape))
    return pl.pallas_call(
        lookup_kernel,
        out_shape=jax.ShapeDtypeStruct((n_micro, tokens, dim), BF16),
        grid_spec=pltpu.PrefetchScalarGridSpec(
            num_scalar_prefetch=1,
            grid=(rows // LOOK_TILE,),
            in_specs=[whole(n_chunk, 1, CHUNK), whole(n_micro, tokens, 1), pl.BlockSpec((dim, LOOK_TILE), lambda i, s: (0, i))],
            out_specs=whole(n_micro, tokens, dim),
            scratch_shapes=[pltpu.VMEM((n_chunk, dim, CHUNK), F32), pltpu.VMEM((n_chunk, dim, CHUNK), BF16)],
        ),
        compiler_params=params(1),
        name="lookup",
    )(starts, ids_rows, rank_cols, table_t)


def peer_copy(src, dst, send, recv, slot, group, stage):
    return pltpu.make_async_remote_copy(
        src_ref=src.at[slot], dst_ref=dst.at[slot], send_sem=send.at[slot], recv_sem=recv.at[slot],
        device_id=(group, stage), device_id_type=MESH)


def greet(group, stage, n_stage):
    barrier = pltpu.get_barrier_semaphore()
    for off in range(1, n_stage):
        pl.semaphore_signal(barrier, inc=1, device_id=(group, lax.rem(stage + off, n_stage)), device_id_type=MESH)
    pl.semaphore_wait(barrier, n_stage - 1)


def each(count, body):
    def step(m, _):
        body(m)
        return 0

    lax.fori_loop(0, count, step, 0)


def gelu_parts(pre):
    inner = jnp.tanh(GELU_A * (pre + GELU_B * pre * pre * pre))
    return inner


def fwd_kernel(part, w1, w2, saved, last, near, far, outbox, acc,
               near_s, near_r, far_s, far_r, act_s, act_r, top_s, top2_s, top_r):
    group, stage = lax.axis_index("dp"), lax.axis_index("stage")
    count = part.shape[0]
    ffn = w1.shape[1]
    greet(group, stage, 4)

    def near_copy(m):
        return peer_copy(part, near, near_s, near_r, m, group, jnp.maximum(stage - 1, 0))

    def far_copy(m):
        return peer_copy(far, far, far_s, far_r, m, group, 0)

    def act_copy(m):
        return peer_copy(outbox, saved, act_s, act_r, m, group, jnp.minimum(stage + 1, 3))

    def top_copy(m, target, sem):
        return peer_copy(last, last, sem, top_r, m, group, target)

    odd = lax.rem(stage, 2) == 1

    @pl.when(odd)
    def _():
        each(count, lambda m: near_copy(m).start())

    @pl.when(stage == 2)
    def _():
        def body(m):
            near_copy(m).wait_recv()
            far[m] = part[m] + near[m]
            far_copy(m).start()

        each(count, body)

    def layer(m):
        @pl.when(stage == 0)
        def _():
            near_copy(m).wait_recv()
            pltpu.make_async_remote_copy(
                src_ref=far.at[m], dst_ref=far.at[m], send_sem=far_s.at[m], recv_sem=far_r.at[m],
                device_id=(group, 2), device_id_type=MESH).wait_recv()
            saved[m] = part[m] + near[m] + far[m]

        @pl.when(stage > 0)
        def _():
            pltpu.make_async_remote_copy(
                src_ref=outbox.at[m], dst_ref=saved.at[m], send_sem=act_s.at[m], recv_sem=act_r.at[m],
                device_id=(group, jnp.maximum(stage - 1, 0)), device_id_type=MESH).wait_recv()

        acts = saved[m]
        for j in range(ffn // FFN_TILE):
            cols = pl.ds(j * FFN_TILE, FFN_TILE)
            pre = mm(acts, w1[:, cols])
            hidden = (0.5 * pre * (1.0 + gelu_parts(pre))).astype(BF16)
            prod = mm(hidden, w2[:, cols], NT)
            if j == 0:
                acc[...] = prod
            else:
                acc[...] += prod
        result = (acts.astype(F32) + acc[...]).astype(BF16)

        @pl.when(stage < 3)
        def _():
            outbox[m] = result
            act_copy(m).start()

        @pl.when(stage == 3)
        def _():
            last[m] = result
            top_copy(m, 1, top_s).start()
            top_copy(m, 2, top2_s).start()

    each(count, layer)

    @pl.when(stage == 1)
    def _():
        def body(m):
            top_copy(m, 0, top_s).wait_recv()
            top_copy(m, 0, top_s).start()

        each(count, body)
        each(count, lambda m: top_copy(m, 0, top_s).wait_send())

    @pl.when(lax.rem(stage, 2) == 0)
    def _():
        each(count, lambda m: top_copy(m, 3, top_s).wait_recv())

    @pl.when(odd)
    def _():
        each(count, lambda m: near_copy(m).wait_send())

    @pl.when(stage == 2)
    def _():
        each(count, lambda m: far_copy(m).wait_send())

    @pl.when(stage < 3)
    def _():
        each(count, lambda m: act_copy(m).wait_send())

    @pl.when(stage == 3)
    def _():
        def body(m):
            top_copy(m, 1, top_s).wait_send()
            top_copy(m, 2, top2_s).wait_send()

        each(count, body)


def run_forward(part, w1, w2):
    count = part.shape[0]
    shape = part.shape
    return pl.pallas_call(
        fwd_kernel,
        out_shape=(jax.ShapeDtypeStruct(shape, BF16), jax.ShapeDtypeStruct(shape, BF16)),
        in_specs=[vmem()] * 3,
        out_specs=(vmem(), vmem()),
        scratch_shapes=[pltpu.VMEM(shape, BF16)] * 3 + [pltpu.VMEM(shape[1:], F32)] + [pltpu.SemaphoreType.DMA((count,))] * 9,
        compiler_params=params(collective_id=0, has_side_effects=True),
        name="forward",
    )(part, w1, w2)


def head_kernel(scale, x_ref, lab_ref, table_ref, prob_ref, norm_ref, max_ref, sum_ref, pick_ref):
    tile_idx = pl.program_id(1)

    @pl.when(tile_idx == 0)
    def _():
        acts = x_ref[...].astype(F32)
        norm_ref[...] = (acts * lax.rsqrt(jnp.mean(acts * acts, axis=-1, keepdims=True) + NORM_EPS)).astype(BF16)
        max_ref[...] = jnp.full(max_ref.shape, jnp.finfo(F32).min, F32)
        sum_ref[...] = jnp.zeros(sum_ref.shape, F32)
        pick_ref[...] = jnp.zeros(pick_ref.shape, F32)

    logits = mm(norm_ref[...], table_ref[...]) * scale
    top = jnp.max(logits, axis=1, keepdims=True)
    prob = jnp.exp(logits - top)
    prob_ref[...] = prob.astype(BF16)
    cols = lax.broadcasted_iota(jnp.int32, logits.shape, 1) + tile_idx * HEAD_TILE
    picked = jnp.sum(jnp.where(cols == lab_ref[...], logits, 0.0), axis=1, keepdims=True)
    here = lax.broadcasted_iota(jnp.int32, max_ref.shape, 1) == tile_idx
    max_ref[...] = jnp.where(here, top, max_ref[...])
    sum_ref[...] = jnp.where(here, jnp.sum(prob, axis=1, keepdims=True), sum_ref[...])
    pick_ref[...] = jnp.where(here, picked, pick_ref[...])


def run_head(acts, labels, table_t, scale):
    tokens, dim = acts.shape
    rows = table_t.shape[1]
    stat = pl.BlockSpec((HEAD_ROWS, 128), lambda i, j: (i, 0))
    return pl.pallas_call(
        functools.partial(head_kernel, scale),
        out_shape=(jax.ShapeDtypeStruct((tokens, rows), BF16), jax.ShapeDtypeStruct((tokens, dim), BF16)) + (jax.ShapeDtypeStruct((tokens, 128), F32),) * 3,
        grid=(tokens // HEAD_ROWS, rows // HEAD_TILE),
        in_specs=[pl.BlockSpec((HEAD_ROWS, dim), lambda i, j: (i, 0)), pl.BlockSpec((HEAD_ROWS, 1), lambda i, j: (i, 0)), pl.BlockSpec((dim, HEAD_TILE), lambda i, j: (0, j))],
        out_specs=(pl.BlockSpec((HEAD_ROWS, HEAD_TILE), lambda i, j: (i, j)), pl.BlockSpec((HEAD_ROWS, dim), lambda i, j: (i, 0)), stat, stat, stat),
        compiler_params=params(2),
        name="head",
    )(acts, labels, table_t)


def head_grad_kernel(prob_ref, coef_ref, lab_ref, lab_coef_ref, table_ref, grad_ref, out_ref, acc):
    tile_idx = pl.program_id(1)
    here = lax.broadcasted_iota(jnp.int32, coef_ref.shape, 1) == tile_idx
    coef = jnp.sum(jnp.where(here, coef_ref[...], 0.0), axis=1, keepdims=True)
    cols = lax.broadcasted_iota(jnp.int32, prob_ref.shape, 1) + tile_idx * HEAD_TILE
    grad = jnp.where(cols == lab_ref[...], lab_coef_ref[...], prob_ref[...].astype(F32) * coef).astype(BF16)
    grad_ref[...] = grad
    prod = mm(grad, table_ref[...], NT)

    @pl.when(tile_idx == 0)
    def _():
        acc[...] = prod

    @pl.when(tile_idx > 0)
    def _():
        acc[...] += prod

    @pl.when(tile_idx == pl.num_programs(1) - 1)
    def _():
        out_ref[...] = acc[...]


def run_head_grad(prob, coef, labels, lab_coef, table_t):
    tokens, rows = prob.shape
    dim = table_t.shape[0]
    tile = pl.BlockSpec((HEAD_ROWS, HEAD_TILE), lambda i, j: (i, j))
    col = pl.BlockSpec((HEAD_ROWS, 1), lambda i, j: (i, 0))
    return pl.pallas_call(
        head_grad_kernel,
        out_shape=(jax.ShapeDtypeStruct((tokens, rows), BF16), jax.ShapeDtypeStruct((tokens, dim), F32)),
        grid=(tokens // HEAD_ROWS, rows // HEAD_TILE),
        in_specs=[tile, pl.BlockSpec((HEAD_ROWS, 128), lambda i, j: (i, 0)), col, col, pl.BlockSpec((dim, HEAD_TILE), lambda i, j: (0, j))],
        out_specs=(tile, pl.BlockSpec((HEAD_ROWS, dim), lambda i, j: (i, 0))),
        scratch_shapes=[pltpu.VMEM((HEAD_ROWS, dim), F32)],
        compiler_params=params(2),
        name="head_grad",
    )(prob, coef, labels, lab_coef, table_t)


def bwd_kernel(gn, last, saved, w1, w2, dy, gx, hid_out, pre_out,
               near, far, outbox, own, hid, dpre, acc,
               near_s, near_r, far_s, far_r, act_s, act_r, low_s, low2_s, low_r, own_sem, hid_sem, pre_sem):
    group, stage = lax.axis_index("dp"), lax.axis_index("stage")
    count = last.shape[0]
    ffn = w1.shape[1]
    greet(group, stage, 4)
    even = lax.rem(stage, 2) == 0

    def near_copy(m):
        return peer_copy(gn, near, near_s, near_r, m, group, jnp.where(even, stage + 1, stage - 1))

    def far_copy(m, target):
        return peer_copy(far, far, far_s, far_r, m, group, target)

    def act_copy(m, target):
        return peer_copy(outbox, dy, act_s, act_r, m, group, target)

    def low_copy(m, target, sem):
        return peer_copy(gx, gx, sem, low_r, m, group, target)

    def own_copy(m):
        return pltpu.make_async_copy(gn.at[m], own.at[lax.rem(m, 2)], own_sem.at[lax.rem(m, 2)])

    def hid_copy(m):
        return pltpu.make_async_copy(hid.at[lax.rem(m, 2)], hid_out.at[m], hid_sem.at[lax.rem(m, 2)])

    def pre_copy(m):
        return pltpu.make_async_copy(dpre.at[lax.rem(m, 2)], pre_out.at[m], pre_sem.at[lax.rem(m, 2)])

    @pl.when(even)
    def _():
        each(count, lambda m: near_copy(m).start())

    @pl.when(jnp.logical_not(even))
    def _():
        own_copy(0).start()

    def next_own(m):
        @pl.when(m + 1 < count)
        def _():
            own_copy(m + 1).start()

        own_copy(m).wait()
        near_copy(m).wait_recv()

    @pl.when(stage == 1)
    def _():
        def body(m):
            next_own(m)
            far[m] = (own[lax.rem(m, 2)] + near[m]).astype(BF16)
            far_copy(m, 3).start()

        each(count, body)

    def layer(m):
        slot = lax.rem(m, 2)

        @pl.when(stage == 3)
        def _():
            next_own(m)
            far_copy(m, 1).wait_recv()
            grad_n = own[slot] + near[m] + far[m].astype(F32)
            acts = last[m].astype(F32)
            inv = lax.rsqrt(jnp.mean(acts * acts, axis=-1, keepdims=True) + NORM_EPS)
            inner = jnp.mean(acts * grad_n, axis=-1, keepdims=True)
            dy[m] = (inv * (grad_n - acts * (inv * inv * inner))).astype(BF16)

        @pl.when(stage < 3)
        def _():
            act_copy(m, jnp.minimum(stage + 1, 3)).wait_recv()

        @pl.when(m >= 2)
        def _():
            hid_copy(m - 2).wait()
            pre_copy(m - 2).wait()

        acts = saved[m]
        grad = dy[m]
        for j in range(ffn // FFN_TILE):
            cols = pl.ds(j * FFN_TILE, FFN_TILE)
            pre = mm(acts, w1[:, cols])
            th = gelu_parts(pre)
            half = 0.5 * (1.0 + th)
            hid[slot, :, cols] = (pre * half).astype(BF16)
            slope = half + 0.5 * pre * (1.0 - th * th) * (GELU_A * (1.0 + 3.0 * GELU_B * pre * pre))
            down = (mm(grad, w2[:, cols]) * slope).astype(BF16)
            dpre[slot, :, cols] = down
            prod = mm(down, w1[:, cols], NT)
            if j == 0:
                acc[...] = prod
            else:
                acc[...] += prod
        result = (grad.astype(F32) + acc[...]).astype(BF16)
        hid_copy(m).start()
        pre_copy(m).start()

        @pl.when(stage > 0)
        def _():
            outbox[m] = result
            act_copy(m, jnp.maximum(stage - 1, 0)).start()

        @pl.when(stage == 0)
        def _():
            gx[m] = result
            low_copy(m, 1, low_s).start()
            low_copy(m, 2, low2_s).start()

    each(count, layer)

    @pl.when(stage == 2)
    def _():
        def body(m):
            low_copy(m, 3, low_s).wait_recv()
            low_copy(m, 3, low_s).start()

        each(count, body)
        each(count, lambda m: low_copy(m, 3, low_s).wait_send())

    @pl.when(jnp.logical_not(even))
    def _():
        each(count, lambda m: low_copy(m, 0, low_s).wait_recv())

    @pl.when(even)
    def _():
        each(count, lambda m: near_copy(m).wait_send())

    @pl.when(stage == 1)
    def _():
        each(count, lambda m: far_copy(m, 3).wait_send())

    @pl.when(stage > 0)
    def _():
        each(count, lambda m: act_copy(m, jnp.maximum(stage - 1, 0)).wait_send())

    @pl.when(stage == 0)
    def _():
        def body(m):
            low_copy(m, 1, low_s).wait_send()
            low_copy(m, 2, low2_s).wait_send()

        each(count, body)

    for m in range(count - 2, count):
        hid_copy(m).wait()
        pre_copy(m).wait()


def run_backward(gn, last, saved, w1, w2):
    shape = saved.shape
    count, tokens, dim = shape
    ffn = w1.shape[1]
    any_spec = pl.BlockSpec(memory_space=pl.ANY)
    wide = jax.ShapeDtypeStruct((count, tokens, ffn), BF16)
    return pl.pallas_call(
        bwd_kernel,
        out_shape=(jax.ShapeDtypeStruct(shape, BF16), jax.ShapeDtypeStruct(shape, BF16), wide, wide),
        in_specs=[any_spec] + [vmem()] * 4,
        out_specs=(vmem(), vmem(), any_spec, any_spec),
        scratch_shapes=[
            pltpu.VMEM(shape, F32), pltpu.VMEM(shape, BF16), pltpu.VMEM(shape, BF16), pltpu.VMEM((2, tokens, dim), F32),
            pltpu.VMEM((2, tokens, ffn), BF16), pltpu.VMEM((2, tokens, ffn), BF16), pltpu.VMEM((tokens, dim), F32),
        ] + [pltpu.SemaphoreType.DMA((count,))] * 9 + [pltpu.SemaphoreType.DMA((2,))] * 3,
        compiler_params=params(collective_id=1, has_side_effects=True),
        name="backward",
    )(gn, last, saved, w1, w2)


def weight_kernel(x_ref, dpre_ref, dy_ref, hid_ref, first_ref, second_ref, xt, dyt):
    @pl.when(pl.program_id(0) == 0)
    def _():
        xt[...] = x_ref[...].T
        dyt[...] = dy_ref[...].T

    first_ref[...] = mm(xt[...], dpre_ref[...])
    second_ref[...] = mm(dyt[...], hid_ref[...])


def run_weights(acts, dpre, dy, hid):
    tokens, dim = acts.shape
    ffn = hid.shape[1]
    whole = pl.BlockSpec((tokens, dim), lambda j: (0, 0))
    tile = pl.BlockSpec((tokens, FFN_TILE), lambda j: (0, j))
    out = pl.BlockSpec((dim, FFN_TILE), lambda j: (0, j))
    return pl.pallas_call(
        weight_kernel,
        out_shape=(jax.ShapeDtypeStruct((dim, ffn), F32),) * 2,
        grid=(ffn // FFN_TILE,),
        in_specs=[whole, tile, whole, tile],
        out_specs=(out, out),
        scratch_shapes=[pltpu.VMEM((dim, tokens), BF16)] * 2,
        compiler_params=params(1),
        name="weights",
    )(acts, dpre, dy, hid)


def table_kernel(starts, ids_ref, rank_ref, norm_ref, gx_ref, grad_ref, out_ref, normt, packed):
    tile_idx = pl.program_id(0)
    n_tiles = pl.num_programs(0)
    n_chunk = packed.shape[0]
    n_micro = gx_ref.shape[0]

    @pl.when(tile_idx == 0)
    def _():
        normt[...] = norm_ref[...].T
        slot = lax.broadcasted_iota(jnp.int32, (rank_ref.shape[1], CHUNK), 1)

        def gather(c, _):
            total = mm(gx_ref[0], one_hot(slot + c * CHUNK == rank_ref[0]), TN)
            for m in range(1, n_micro):
                total += mm(gx_ref[m], one_hot(slot + c * CHUNK == rank_ref[m]), TN)
            packed[c] = total.astype(BF16)
            return 0

        lax.fori_loop(0, n_chunk, gather, 0)

    out_ref[...] = mm(normt[...], grad_ref[...])
    first, last = chunk_bounds(starts, tile_idx)
    base = starts[n_tiles + 1] + tile_idx * LOOK_TILE

    def step(c, _):
        rows = lax.broadcasted_iota(jnp.int32, (CHUNK, LOOK_TILE), 1) + base
        out_ref[...] += mm(packed[c], one_hot(rows == ids_ref[c]))
        return 0

    lax.fori_loop(first, last, step, 0)


def run_table(starts, ids_cols, rank_cols, normed, gx, grad):
    tokens, rows = grad.shape
    n_micro, micro, dim = gx.shape
    n_chunk = tokens // CHUNK
    whole = lambda *shape: pl.BlockSpec(shape, lambda i, s: (0,) * len(shape))
    return pl.pallas_call(
        table_kernel,
        out_shape=jax.ShapeDtypeStruct((dim, rows), F32),
        grid_spec=pltpu.PrefetchScalarGridSpec(
            num_scalar_prefetch=1,
            grid=(rows // LOOK_TILE,),
            in_specs=[whole(n_chunk, CHUNK, 1), whole(n_micro, micro, 1), whole(tokens, dim), whole(n_micro, micro, dim), pl.BlockSpec((tokens, LOOK_TILE), lambda i, s: (0, i))],
            out_specs=pl.BlockSpec((dim, LOOK_TILE), lambda i, s: (0, i)),
            scratch_shapes=[pltpu.VMEM((dim, tokens), BF16), pltpu.VMEM((n_chunk, dim, CHUNK), BF16)],
        ),
        compiler_params=params(1),
        name="table",
    )(starts, ids_cols, rank_cols, normed, gx, grad)


def solution(mesh):
    def body(token_ids, label_ids, emb_rows, w_in, w_out):
        stage = lax.axis_index("stage")
        n_micro, micro = token_ids.shape
        rows, dim = emb_rows.shape
        tokens = n_micro * micro
        scale = dim ** -0.5
        row_start = stage * rows
        table_t = emb_rows.T
        w1 = w_in[0]
        w2 = w_out[0].T

        flat = token_ids.reshape(-1)
        order_key = flat * tokens + jnp.arange(tokens, dtype=jnp.int32)
        rank = jnp.sum((order_key[None, :] < order_key[:, None]).astype(jnp.int32), axis=1)
        sorted_ids = jnp.sort(order_key) // tokens
        edges = row_start + jnp.arange(rows // LOOK_TILE + 1, dtype=jnp.int32) * LOOK_TILE
        starts = jnp.sum((flat[None, :] < edges[:, None]).astype(jnp.int32), axis=1)
        starts = jnp.concatenate([starts, row_start[None]]).astype(jnp.int32)
        rank_cols = rank.reshape(n_micro, micro, 1)
        ids_rows = sorted_ids.reshape(-1, 1, CHUNK)
        ids_cols = sorted_ids.reshape(-1, CHUNK, 1)

        part = run_lookup(starts, ids_rows, rank_cols, table_t)
        saved, last = run_forward(part, w1, w2)

        labels = (label_ids - row_start).reshape(tokens, 1)
        prob, normed, tile_max, tile_sum, tile_pick = run_head(last.reshape(tokens, dim), labels, table_t, scale)
        top = jnp.max(tile_max, axis=1)
        total = jnp.sum(tile_sum * jnp.exp(tile_max - top[:, None]), axis=1)
        stats = lax.all_gather(jnp.stack([top, total, jnp.sum(tile_pick, axis=1)]), "stage")
        row_max = jnp.max(stats[:, 0], axis=0)
        row_sum = jnp.sum(stats[:, 1] * jnp.exp(stats[:, 0] - row_max), axis=0)
        picked = jnp.sum(stats[:, 2], axis=0)
        loss = jnp.sum(jnp.log(row_sum) + row_max - picked) / tokens
        coef = jnp.exp(tile_max - row_max[:, None]) / row_sum[:, None] * scale
        lab_coef = (jnp.exp(picked - row_max) / row_sum - 1.0) * scale
        grad, grad_n = run_head_grad(prob, coef, labels, lab_coef[:, None], table_t)

        dy, gx, hid, dpre = run_backward(grad_n.reshape(n_micro, micro, dim), last, saved, w1, w2)
        flatten = lambda arr: arr.reshape(tokens, arr.shape[-1])
        grad_first, grad_second = run_weights(flatten(saved), flatten(dpre), flatten(dy), flatten(hid))
        grad_table = run_table(starts, ids_cols, rank_cols, normed, gx, grad)
        return loss.reshape(1), grad_first[None], grad_second.T[None], grad_table.T

    return jax.shard_map(
        body,
        mesh=mesh,
        in_specs=(P("dp", None), P("dp", None), P("stage", None), P("stage", None, None), P("stage", None, None)),
        out_specs=(P("dp"), P(("dp", "stage"), None, None), P(("dp", "stage"), None, None), P(("dp", "stage"), None)),
        check_vma=False,
    )
```

```python
import functools

import jax
import jax.numpy as jnp
from jax import lax
from jax.experimental import pallas as pl
from jax.experimental.pallas import tpu as pltpu
from jax.sharding import PartitionSpec as P

NORM_EPS = 1e-6
GELU_A = 0.7978845608028654
GELU_B = 0.044715
NN = (((1,), (0,)), ((), ()))
NT = (((1,), (1,)), ((), ()))
TN = (((0,), (0,)), ((), ()))
MESH = pl.DeviceIdType.MESH
BF16 = jnp.bfloat16
F32 = jnp.float32
VMEM_ALL = 66_000_000
CHUNK = 256
LOOK_TILE = 512
LOOK_STEP = 2048
OUT_TILE = 1024
PASS_TILE = 256
HEAD_MICRO = 2
HEAD_TILE = 2048
HEAD_SUB = 256
GRAD_ROWS = 1024
GRAD_SUB = 256
GRAD_TILE = 3072
LOG2_E = 1.4426950408889634
FFN_TILE = 512


def mm(lhs, rhs, dims=NN):
    return lax.dot_general(lhs, rhs, dims, preferred_element_type=F32)


def one_hot(match):
    return jnp.where(match, 1.0, 0.0).astype(BF16)


def params(n_axes=0, **kwargs):
    if n_axes:
        kwargs["dimension_semantics"] = ("arbitrary",) * n_axes
    kwargs.setdefault("vmem_limit_bytes", VMEM_ALL)
    return pltpu.CompilerParams(**kwargs)


def vmem():
    return pl.BlockSpec(memory_space=pltpu.VMEM)


def chunk_bounds(starts, tile_idx, width=1):
    lo, hi = starts[tile_idx * width], starts[(tile_idx + 1) * width]
    first = lo // CHUNK
    return first, jnp.where(hi > lo, (hi + CHUNK - 1) // CHUNK, first)


def lookup_kernel(starts, ids_ref, rank_ref, table_ref, out_ref, acc, packed, total):
    tile_idx = pl.program_id(0)
    n_tiles = pl.num_programs(0)
    @pl.when(tile_idx == 0)
    def _():
        acc[...] = jnp.zeros_like(acc)

    first, last = chunk_bounds(starts, tile_idx, LOOK_STEP // LOOK_TILE)
    base = starts[starts.shape[0] - 1] + tile_idx * LOOK_STEP

    def step(c, _):
        rows = lax.broadcasted_iota(jnp.int32, (LOOK_STEP, CHUNK), 0) + base
        acc[c] += mm(table_ref[...], one_hot(rows == ids_ref[c]))
        return 0

    lax.fori_loop(first, last, step, 0)

    @pl.when(tile_idx == n_tiles - 1)
    def _():
        slot = lax.broadcasted_iota(jnp.int32, (rank_ref.shape[1], CHUNK), 1)
        used_first, used_last = chunk_bounds(starts, 0, starts.shape[0] - 2)

        def pack(c, _):
            packed[c] = acc[c].astype(BF16)
            return 0

        lax.fori_loop(used_first, used_last, pack, 0)

        def back(m, _):
            total[...] = jnp.zeros_like(total)

            def add(c, _):
                total[...] += mm(one_hot(slot + c * CHUNK == rank_ref[m]), packed[c], NT)
                return 0

            lax.fori_loop(used_first, used_last, add, 0)
            out_ref[m] = total[...].astype(BF16)
            return 0

        lax.fori_loop(0, out_ref.shape[0], back, 0)


def run_lookup(starts, ids_rows, rank_cols, table_t):
    dim, rows = table_t.shape
    n_micro, tokens = rank_cols.shape[:2]
    n_chunk = n_micro * tokens // CHUNK
    whole = lambda *shape: pl.BlockSpec(shape, lambda i, s: (0,) * len(shape))
    return pl.pallas_call(
        lookup_kernel,
        out_shape=jax.ShapeDtypeStruct((n_micro, tokens, dim), BF16),
        grid_spec=pltpu.PrefetchScalarGridSpec(
            num_scalar_prefetch=1,
            grid=(rows // LOOK_STEP,),
            in_specs=[whole(n_chunk, 1, CHUNK), whole(n_micro, tokens, 1), pl.BlockSpec((dim, LOOK_STEP), lambda i, s: (0, i))],
            out_specs=whole(n_micro, tokens, dim),
            scratch_shapes=[pltpu.VMEM((n_chunk, dim, CHUNK), F32), pltpu.VMEM((n_chunk, dim, CHUNK), BF16), pltpu.VMEM((tokens, dim), F32)],
        ),
        compiler_params=params(1),
        name="lookup",
    )(starts, ids_rows, rank_cols, table_t)


def peer_copy(src, dst, send, recv, slot, group, stage):
    return pltpu.make_async_remote_copy(
        src_ref=src.at[slot], dst_ref=dst.at[slot], send_sem=send.at[slot], recv_sem=recv.at[slot],
        device_id=(group, stage), device_id_type=MESH)


def greet(group, stage, n_stage):
    barrier = pltpu.get_barrier_semaphore()
    for off in range(1, n_stage):
        pl.semaphore_signal(barrier, inc=1, device_id=(group, lax.rem(stage + off, n_stage)), device_id_type=MESH)
    pl.semaphore_wait(barrier, n_stage - 1)


def each(count, body):
    def step(m, _):
        body(m)
        return 0

    lax.fori_loop(0, count, step, 0)


def gelu_parts(pre):
    inner = jnp.tanh(GELU_A * (pre + GELU_B * pre * pre * pre))
    return inner


def fwd_kernel(scale, part, w1, w2, labels, table, saved, last, tile_max, tile_sum, tile_pick, prob_out,
               near, far, outbox, acc, normed, rows_buf, prob_buf,
               near_s, near_r, far_s, far_r, act_s, act_r, top_s, top2_s, top_r, rows_sem, prob_sem):
    group, stage = lax.axis_index("dp"), lax.axis_index("stage")
    count, micro = part.shape[:2]
    block = HEAD_MICRO * micro
    n_block = count // HEAD_MICRO
    n_tiles = table.shape[1] // HEAD_TILE
    n_sub = HEAD_TILE // HEAD_SUB

    def rows_copy(step):
        return pltpu.make_async_copy(
            table.at[:, pl.ds(pl.multiple_of(lax.rem(step, n_tiles) * HEAD_TILE, HEAD_TILE), HEAD_TILE)],
            rows_buf.at[lax.rem(step, 2)], rows_sem.at[lax.rem(step, 2)])

    def prob_copy(step):
        return pltpu.make_async_copy(
            prob_buf.at[lax.rem(step, 2)],
            prob_out.at[pl.ds(pl.multiple_of(step // n_tiles * block, block), block), pl.ds(pl.multiple_of(lax.rem(step, n_tiles) * HEAD_TILE, HEAD_TILE), HEAD_TILE)],
            prob_sem.at[lax.rem(step, 2)])

    rows_copy(0).start()
    ffn = w1.shape[1]
    greet(group, stage, 4)

    def near_copy(m):
        return peer_copy(part, near, near_s, near_r, m, group, jnp.maximum(stage - 1, 0))

    def far_copy(m):
        return peer_copy(far, far, far_s, far_r, m, group, 0)

    def act_copy(m):
        return peer_copy(outbox, saved, act_s, act_r, m, group, jnp.minimum(stage + 1, 3))

    def top_copy(m, target, sem):
        return peer_copy(last, last, sem, top_r, m, group, target)

    odd = lax.rem(stage, 2) == 1

    @pl.when(odd)
    def _():
        each(count, lambda m: near_copy(m).start())

    @pl.when(stage == 2)
    def _():
        def body(m):
            near_copy(m).wait_recv()
            far[m] = part[m] + near[m]
            far_copy(m).start()

        each(count, body)

    def layer(m):
        @pl.when(stage == 0)
        def _():
            near_copy(m).wait_recv()
            pltpu.make_async_remote_copy(
                src_ref=far.at[m], dst_ref=far.at[m], send_sem=far_s.at[m], recv_sem=far_r.at[m],
                device_id=(group, 2), device_id_type=MESH).wait_recv()
            saved[m] = part[m] + near[m] + far[m]

        @pl.when(stage > 0)
        def _():
            pltpu.make_async_remote_copy(
                src_ref=outbox.at[m], dst_ref=saved.at[m], send_sem=act_s.at[m], recv_sem=act_r.at[m],
                device_id=(group, jnp.maximum(stage - 1, 0)), device_id_type=MESH).wait_recv()

        acts = saved[m]
        for j in range(ffn // FFN_TILE):
            cols = pl.ds(j * FFN_TILE, FFN_TILE)
            pre = mm(acts, w1[:, cols])
            hidden = (0.5 * pre * (1.0 + gelu_parts(pre))).astype(BF16)
            prod = mm(hidden, w2[:, cols], NT)
            if j == 0:
                acc[...] = prod
            else:
                acc[...] += prod
        result = (acts.astype(F32) + acc[...]).astype(BF16)

        @pl.when(stage < 3)
        def _():
            outbox[m] = result
            act_copy(m).start()

        @pl.when(stage == 3)
        def _():
            last[m] = result
            top_copy(m, 1, top_s).start()
            top_copy(m, 2, top2_s).start()

    def head_tile(step):
        slot = lax.rem(step, 2)
        rows = pl.ds(pl.multiple_of(step // n_tiles * block, block), block)
        tile_idx = lax.rem(step, n_tiles)

        @pl.when(step + 1 < n_block * n_tiles)
        def _():
            rows_copy(step + 1).start()

        rows_copy(step).wait()

        @pl.when(step >= 2)
        def _():
            prob_copy(step - 2).wait()

        acts = normed[...]
        lane = lax.broadcasted_iota(jnp.int32, (block, 128), 1)
        cols = lax.broadcasted_iota(jnp.int32, (block, HEAD_SUB), 1)
        tops, sums, picks = tile_max[rows, :], tile_sum[rows, :], tile_pick[rows, :]
        for q in range(n_sub):
            sub = pl.ds(q * HEAD_SUB, HEAD_SUB)
            raw = mm(acts, rows_buf[slot, :, sub])
            top = jnp.max(raw, axis=1, keepdims=True)
            prob = jnp.exp2((raw - top) * (scale * LOG2_E))
            prob_buf[slot, :, sub] = prob.astype(BF16)
            match = cols == labels[rows, :] - (tile_idx * HEAD_TILE + q * HEAD_SUB)
            picked = jnp.sum(jnp.where(match, raw, 0.0), axis=1, keepdims=True)
            here = lane == tile_idx * n_sub + q
            tops = jnp.where(here, top * scale, tops)
            sums = jnp.where(here, jnp.sum(prob, axis=1, keepdims=True), sums)
            picks = jnp.where(here, picked * scale, picks)
        tile_max[rows, :], tile_sum[rows, :], tile_pick[rows, :] = tops, sums, picks
        prob_copy(step).start()

    def head_block(b):
        for i in range(HEAD_MICRO):
            m = b * HEAD_MICRO + i

            @pl.when(stage == 1)
            def _():
                top_copy(m, 0, top_s).wait_recv()
                top_copy(m, 0, top_s).start()

            @pl.when(lax.rem(stage, 2) == 0)
            def _():
                top_copy(m, 3, top_s).wait_recv()

            acts = last[m].astype(F32)
            inv = lax.rsqrt(jnp.mean(acts * acts, axis=-1, keepdims=True) + NORM_EPS)
            normed[pl.ds(i * micro, micro), :] = (acts * inv).astype(BF16)

        each(n_tiles, lambda j: head_tile(b * n_tiles + j))

    tile_max[...] = jnp.full(tile_max.shape, jnp.finfo(F32).min, F32)
    tile_sum[...] = jnp.zeros(tile_sum.shape, F32)
    tile_pick[...] = jnp.zeros(tile_pick.shape, F32)
    first_head = jnp.where(stage == 3, count // 2, jnp.where(stage == 2, count // 2 + 1, count))

    def work(k):
        head = jnp.logical_or(k == first_head, k > count)

        @pl.when(head)
        def _():
            head_block(jnp.maximum(k - count, 0))

        @pl.when(jnp.logical_not(head))
        def _():
            layer(jnp.where(k < first_head, k, k - 1))

    each(count + n_block, work)
    for step in range(n_block * n_tiles - 2, n_block * n_tiles):
        prob_copy(step).wait()

    @pl.when(stage == 1)
    def _():
        each(count, lambda m: top_copy(m, 0, top_s).wait_send())

    @pl.when(odd)
    def _():
        each(count, lambda m: near_copy(m).wait_send())

    @pl.when(stage == 2)
    def _():
        each(count, lambda m: far_copy(m).wait_send())

    @pl.when(stage < 3)
    def _():
        each(count, lambda m: act_copy(m).wait_send())

    @pl.when(stage == 3)
    def _():
        def body(m):
            top_copy(m, 1, top_s).wait_send()
            top_copy(m, 2, top2_s).wait_send()

        each(count, body)


def run_forward(part, w1, w2, labels, table_t, scale):
    count, micro, dim = part.shape
    shape = part.shape
    rows = table_t.shape[1]
    block = HEAD_MICRO * micro
    any_spec = pl.BlockSpec(memory_space=pl.ANY)
    stat = jax.ShapeDtypeStruct((count * micro, 128), F32)
    return pl.pallas_call(
        functools.partial(fwd_kernel, scale),
        out_shape=(jax.ShapeDtypeStruct(shape, BF16), jax.ShapeDtypeStruct(shape, BF16), stat, stat, stat, jax.ShapeDtypeStruct((count * micro, rows), BF16)),
        in_specs=[vmem()] * 4 + [any_spec],
        out_specs=(vmem(),) * 5 + (any_spec,),
        scratch_shapes=[pltpu.VMEM(shape, BF16)] * 3 + [
            pltpu.VMEM((micro, dim), F32), pltpu.VMEM((block, dim), BF16), pltpu.VMEM((2, dim, HEAD_TILE), BF16), pltpu.VMEM((2, block, HEAD_TILE), BF16),
        ] + [pltpu.SemaphoreType.DMA((count,))] * 9 + [pltpu.SemaphoreType.DMA((2,))] * 2,
        compiler_params=params(collective_id=0, has_side_effects=True),
        name="forward",
    )(part, w1, w2, labels, table_t)


def head_grad_kernel(prob_ref, coef_ref, lab_ref, lab_coef_ref, table_ref, grad_ref, out_ref, acc):
    tile_idx = pl.program_id(1)
    n_sub = GRAD_TILE // HEAD_SUB

    @pl.when(tile_idx == 0)
    def _():
        acc[...] = jnp.zeros_like(acc)

    lane = lax.broadcasted_iota(jnp.int32, (GRAD_SUB, 128), 1)
    cols = lax.broadcasted_iota(jnp.int32, (GRAD_SUB, HEAD_SUB), 1)
    for r in range(GRAD_ROWS // GRAD_SUB):
        rows = pl.ds(r * GRAD_SUB, GRAD_SUB)
        coefs = coef_ref[rows, :]
        pieces = []
        for q in range(n_sub):
            sub = pl.ds(q * HEAD_SUB, HEAD_SUB)
            coef = jnp.sum(jnp.where(lane == tile_idx * n_sub + q, coefs, 0.0), axis=1, keepdims=True)
            match = cols == lab_ref[rows, :] - (tile_idx * GRAD_TILE + q * HEAD_SUB)
            grad = jnp.where(match, lab_coef_ref[rows, :], prob_ref[rows, sub].astype(F32) * coef).astype(BF16)
            grad_ref[rows, sub] = grad
            pieces.append(grad)
        acc[rows, :] += mm(jnp.concatenate(pieces, axis=1), table_ref[...], NT)

    @pl.when(tile_idx == pl.num_programs(1) - 1)
    def _():
        out_ref[...] = acc[...]


def run_head_grad(prob, coef, labels, lab_coef, table_t):
    tokens, rows = prob.shape
    dim = table_t.shape[0]
    tile = pl.BlockSpec((GRAD_ROWS, GRAD_TILE), lambda i, j: (i, j))
    col = pl.BlockSpec((GRAD_ROWS, 1), lambda i, j: (i, 0))
    return pl.pallas_call(
        head_grad_kernel,
        out_shape=(jax.ShapeDtypeStruct((tokens, rows), BF16), jax.ShapeDtypeStruct((tokens, dim), F32)),
        grid=(tokens // GRAD_ROWS, rows // GRAD_TILE),
        in_specs=[tile, pl.BlockSpec((GRAD_ROWS, 128), lambda i, j: (i, 0)), col, col, pl.BlockSpec((dim, GRAD_TILE), lambda i, j: (0, j))],
        out_specs=(tile, pl.BlockSpec((GRAD_ROWS, dim), lambda i, j: (i, 0))),
        scratch_shapes=[pltpu.VMEM((GRAD_ROWS, dim), F32)],
        compiler_params=params(2),
        name="head_grad",
    )(prob, coef, labels, lab_coef, table_t)


def bwd_kernel(gn, last, saved, w1, w2, gx, first, second,
               near, far, dy, outbox, own, top, acts_buf, hid, dpre, acc,
               near_s, near_r, far_s, far_r, act_s, act_r, low_s, low2_s, low_r, own_sem, top_sem, acts_sem):
    group, stage = lax.axis_index("dp"), lax.axis_index("stage")
    count = near.shape[0]
    ffn = w1.shape[1]
    even = lax.rem(stage, 2) == 0

    def local_copy(src, dst, sem, m):
        return pltpu.make_async_copy(src.at[m], dst.at[lax.rem(m, 2)], sem.at[lax.rem(m, 2)])

    def near_copy(m):
        return peer_copy(gn, near, near_s, near_r, m, group, jnp.where(even, stage + 1, stage - 1))

    def far_copy(m, target):
        return peer_copy(far, far, far_s, far_r, m, group, target)

    def act_copy(m, target):
        return pltpu.make_async_remote_copy(
            src_ref=outbox.at[lax.rem(m, 2)], dst_ref=dy.at[m], send_sem=act_s.at[m], recv_sem=act_r.at[m],
            device_id=(group, target), device_id_type=MESH)

    def low_copy(m, target, sem):
        return peer_copy(gx, gx, sem, low_r, m, group, target)

    def own_copy(m):
        return local_copy(gn, own, own_sem, m)

    def top_copy(m):
        return local_copy(last, top, top_sem, m)

    def acts_copy(m):
        return local_copy(saved, acts_buf, acts_sem, m)

    acts_copy(0).start()

    @pl.when(stage == 3)
    def _():
        top_copy(0).start()

    @pl.when(jnp.logical_not(even))
    def _():
        own_copy(0).start()

    greet(group, stage, 4)

    @pl.when(even)
    def _():
        each(count, lambda m: near_copy(m).start())

    first[...] = jnp.zeros_like(first)
    second[...] = jnp.zeros_like(second)

    def advance(copy, m):
        @pl.when(m + 1 < count)
        def _():
            copy(m + 1).start()

        copy(m).wait()

    @pl.when(stage == 1)
    def _():
        def body(m):
            advance(own_copy, m)
            near_copy(m).wait_recv()
            far[m] = (own[lax.rem(m, 2)] + near[m]).astype(BF16)
            far_copy(m, 3).start()

        each(count, body)

    def layer(m):
        slot = lax.rem(m, 2)
        advance(acts_copy, m)

        @pl.when(stage == 3)
        def _():
            advance(own_copy, m)
            advance(top_copy, m)
            near_copy(m).wait_recv()
            far_copy(m, 1).wait_recv()
            grad_n = own[slot] + near[m] + far[m].astype(F32)
            acts = top[slot].astype(F32)
            inv = lax.rsqrt(jnp.mean(acts * acts, axis=-1, keepdims=True) + NORM_EPS)
            inner = jnp.mean(acts * grad_n, axis=-1, keepdims=True)
            dy[m] = (inv * (grad_n - acts * (inv * inv * inner))).astype(BF16)

        @pl.when(stage < 3)
        def _():
            act_copy(m, jnp.minimum(stage + 1, 3)).wait_recv()

        acts = acts_buf[slot]
        grad = dy[m]
        for j in range(ffn // FFN_TILE):
            cols = pl.ds(j * FFN_TILE, FFN_TILE)
            pre = mm(acts, w1[:, cols])
            th = gelu_parts(pre)
            half = 0.5 * (1.0 + th)
            hid[:, cols] = (pre * half).astype(BF16)
            slope = half + 0.5 * pre * (1.0 - th * th) * (GELU_A * (1.0 + 3.0 * GELU_B * pre * pre))
            down = (mm(grad, w2[:, cols]) * slope).astype(BF16)
            dpre[:, cols] = down
            prod = mm(down, w1[:, cols], NT)
            if j == 0:
                acc[...] = prod
            else:
                acc[...] += prod
        result = (grad.astype(F32) + acc[...]).astype(BF16)

        @pl.when(stage > 0)
        def _():
            @pl.when(m >= 2)
            def _():
                act_copy(m - 2, jnp.maximum(stage - 1, 0)).wait_send()

            outbox[slot] = result
            act_copy(m, jnp.maximum(stage - 1, 0)).start()

        @pl.when(stage == 0)
        def _():
            gx[m] = result
            low_copy(m, 1, low_s).start()
            low_copy(m, 2, low2_s).start()

        acts_t, grad_t = acts.T, grad.T
        for j in range(ffn // FFN_TILE):
            cols = pl.ds(j * FFN_TILE, FFN_TILE)
            first[:, cols] += mm(acts_t, dpre[:, cols])
            second[:, cols] += mm(grad_t, hid[:, cols])

    each(count, layer)

    @pl.when(stage == 2)
    def _():
        def body(m):
            low_copy(m, 3, low_s).wait_recv()
            low_copy(m, 3, low_s).start()

        each(count, body)
        each(count, lambda m: low_copy(m, 3, low_s).wait_send())

    @pl.when(jnp.logical_not(even))
    def _():
        each(count, lambda m: low_copy(m, 0, low_s).wait_recv())

    @pl.when(even)
    def _():
        each(count, lambda m: near_copy(m).wait_send())

    @pl.when(stage == 1)
    def _():
        each(count, lambda m: far_copy(m, 3).wait_send())

    @pl.when(stage > 0)
    def _():
        for m in range(count - 2, count):
            act_copy(m, jnp.maximum(stage - 1, 0)).wait_send()

    @pl.when(stage == 0)
    def _():
        def body(m):
            low_copy(m, 1, low_s).wait_send()
            low_copy(m, 2, low2_s).wait_send()

        each(count, body)


def run_backward(gn, last, saved, w1, w2):
    shape = saved.shape
    count, tokens, dim = shape
    ffn = w1.shape[1]
    any_spec = pl.BlockSpec(memory_space=pl.ANY)
    pair = lambda dtype: pltpu.VMEM((2, tokens, dim), dtype)
    return pl.pallas_call(
        bwd_kernel,
        out_shape=(jax.ShapeDtypeStruct(shape, BF16), jax.ShapeDtypeStruct((dim, ffn), F32), jax.ShapeDtypeStruct((dim, ffn), F32)),
        in_specs=[any_spec] * 3 + [vmem()] * 2,
        out_specs=(vmem(),) * 3,
        scratch_shapes=[
            pltpu.VMEM(shape, F32), pltpu.VMEM(shape, BF16), pltpu.VMEM(shape, BF16), pair(BF16), pair(F32), pair(BF16), pair(BF16),
            pltpu.VMEM((tokens, ffn), BF16), pltpu.VMEM((tokens, ffn), BF16), pltpu.VMEM((tokens, dim), F32),
        ] + [pltpu.SemaphoreType.DMA((count,))] * 9 + [pltpu.SemaphoreType.DMA((2,))] * 3,
        compiler_params=params(collective_id=1, has_side_effects=True),
        name="backward",
    )(gn, last, saved, w1, w2)


def table_kernel(starts, ids_ref, rank_ref, last_ref, gx_ref, grad_ref, first_ref, second_ref, out_ref, first_out, second_out, normt, packed):
    tile_idx = pl.program_id(0)
    n_chunk = packed.shape[0]
    n_micro = gx_ref.shape[0]

    @pl.when(tile_idx == 0)
    def _():
        for m in range(n_micro):
            acts = last_ref[m].astype(F32)
            inv = lax.rsqrt(jnp.mean(acts * acts, axis=-1, keepdims=True) + NORM_EPS)
            normt[:, m * acts.shape[0]:(m + 1) * acts.shape[0]] = (acts * inv).astype(BF16).T

        slot = lax.broadcasted_iota(jnp.int32, (rank_ref.shape[1], CHUNK), 1)

        packed[...] = jnp.zeros_like(packed)

        def gather(c, _):
            total = mm(gx_ref[0], one_hot(slot + c * CHUNK == rank_ref[0]), TN)
            for m in range(1, n_micro):
                total += mm(gx_ref[m], one_hot(slot + c * CHUNK == rank_ref[m]), TN)
            packed[c] = total.astype(BF16)
            return 0

        used_first, used_last = chunk_bounds(starts, 0, starts.shape[0] - 2)
        lax.fori_loop(used_first, used_last, gather, 0)

    first, last = chunk_bounds(starts, tile_idx, OUT_TILE // LOOK_TILE)
    base = starts[starts.shape[0] - 1] + tile_idx * OUT_TILE
    rows = lax.broadcasted_iota(jnp.int32, (CHUNK, OUT_TILE), 1) + base
    near = jnp.minimum(first, n_chunk - 1)
    out_ref[...] = mm(normt[...], grad_ref[...]) + mm(packed[near], one_hot(rows == ids_ref[near]))
    first_out[...] = first_ref[...]
    second_out[...] = second_ref[...]

    def step(c, _):
        out_ref[...] += mm(packed[c], one_hot(rows == ids_ref[c]))
        return 0

    lax.fori_loop(first + 1, last, step, 0)


def run_table(starts, ids_cols, rank_cols, last, gx, grad, first, second):
    tokens, rows = grad.shape
    n_micro, micro, dim = gx.shape
    n_chunk = tokens // CHUNK
    steps = rows // OUT_TILE
    width = PASS_TILE
    passed = pl.BlockSpec((dim, width), lambda i, s: (0, jnp.minimum(i, first.shape[1] // width - 1)))
    whole = lambda *shape: pl.BlockSpec(shape, lambda i, s: (0,) * len(shape))
    return pl.pallas_call(
        table_kernel,
        out_shape=(jax.ShapeDtypeStruct((dim, rows), F32),) + (jax.ShapeDtypeStruct(first.shape, F32),) * 2,
        grid_spec=pltpu.PrefetchScalarGridSpec(
            num_scalar_prefetch=1,
            grid=(steps,),
            in_specs=[whole(n_chunk, CHUNK, 1), whole(n_micro, micro, 1), whole(n_micro, micro, dim), whole(n_micro, micro, dim), pl.BlockSpec((tokens, OUT_TILE), lambda i, s: (0, i)), passed, passed],
            out_specs=(pl.BlockSpec((dim, OUT_TILE), lambda i, s: (0, i)), passed, passed),
            scratch_shapes=[pltpu.VMEM((dim, tokens), BF16), pltpu.VMEM((n_chunk, dim, CHUNK), BF16)],
        ),
        compiler_params=params(1),
        name="table",
    )(starts, ids_cols, rank_cols, last, gx, grad, first, second)


def solution(mesh):
    def body(token_ids, label_ids, emb_rows, w_in, w_out):
        stage = lax.axis_index("stage")
        n_micro, micro = token_ids.shape
        rows, dim = emb_rows.shape
        tokens = n_micro * micro
        scale = dim ** -0.5
        row_start = stage * rows
        table_t = emb_rows.T
        w1 = w_in[0]
        w2 = w_out[0].T

        flat = token_ids.reshape(-1)
        order_key = flat * tokens + jnp.arange(tokens, dtype=jnp.int32)
        rank = jnp.sum((order_key[None, :] < order_key[:, None]).astype(jnp.int32), axis=1)
        slots = jnp.arange(tokens, dtype=jnp.int32)
        sorted_ids = jnp.sum(jnp.where(rank[None, :] == slots[:, None], flat[None, :], 0), axis=1)
        edges = row_start + jnp.arange(rows // LOOK_TILE + 1, dtype=jnp.int32) * LOOK_TILE
        starts = jnp.sum((flat[None, :] < edges[:, None]).astype(jnp.int32), axis=1)
        starts = jnp.concatenate([starts, row_start[None]]).astype(jnp.int32)
        rank_cols = rank.reshape(n_micro, micro, 1)
        ids_rows = sorted_ids.reshape(-1, 1, CHUNK)
        ids_cols = sorted_ids.reshape(-1, CHUNK, 1)

        part = run_lookup(starts, ids_rows, rank_cols, table_t)
        labels = (label_ids - row_start).reshape(tokens, 1)
        saved, last, tile_max, tile_sum, tile_pick, prob = run_forward(part, w1, w2, labels, table_t, scale)
        top = jnp.max(tile_max, axis=1)
        total = jnp.sum(tile_sum * jnp.exp(tile_max - top[:, None]), axis=1)
        stats = lax.all_gather(jnp.stack([top, total, jnp.sum(tile_pick, axis=1)]), "stage")
        row_max = jnp.max(stats[:, 0], axis=0)
        row_sum = jnp.sum(stats[:, 1] * jnp.exp(stats[:, 0] - row_max), axis=0)
        picked = jnp.sum(stats[:, 2], axis=0)
        loss = jnp.sum(jnp.log(row_sum) + row_max - picked) / tokens
        coef = jnp.exp(tile_max - row_max[:, None]) / row_sum[:, None] * scale
        lab_coef = (jnp.exp(picked - row_max) / row_sum - 1.0) * scale
        grad, grad_n = run_head_grad(prob, coef, labels, lab_coef[:, None], table_t)

        gx, grad_first, grad_second = run_backward(grad_n.reshape(n_micro, micro, dim), last, saved, w1, w2)
        grad_table, grad_first, grad_second = run_table(starts, ids_cols, rank_cols, last, gx, grad, grad_first, grad_second)
        return loss.reshape(1), grad_first[None], grad_second.T[None], grad_table.T

    return jax.shard_map(
        body,
        mesh=mesh,
        in_specs=(P("dp", None), P("dp", None), P("stage", None), P("stage", None, None), P("stage", None, None)),
        out_specs=(P("dp"), P(("dp", "stage"), None, None), P(("dp", "stage"), None, None), P(("dp", "stage"), None)),
        check_vma=False,
    )
```

```python
import functools

import jax
import jax.numpy as jnp
from jax import lax
from jax.experimental import pallas as pl
from jax.experimental.pallas import tpu as pltpu
from jax.sharding import PartitionSpec as P

NORM_EPS = 1e-6
GELU_A = 0.7978845608028654
GELU_B = 0.044715
NN = (((1,), (0,)), ((), ()))
NT = (((1,), (1,)), ((), ()))
TN = (((0,), (0,)), ((), ()))
MESH = pl.DeviceIdType.MESH
BF16 = jnp.bfloat16
F32 = jnp.float32
VMEM_ALL = 66_000_000
CHUNK = 256
LOOK_TILE = 512
LOOK_STEP = 2048
OUT_TILE = 1024
PASS_TILE = 256
HEAD_MICRO = 2
HEAD_TILE = 3072
HEAD_SUB = 256
GRAD_ROWS = 1024
GRAD_SUB = 512
GRAD_TILE = 2048
LOG2_E = 1.4426950408889634
FFN_TILE = 512


def mm(lhs, rhs, dims=NN):
    return lax.dot_general(lhs, rhs, dims, preferred_element_type=F32)


def one_hot(match):
    return jnp.where(match, 1.0, 0.0).astype(BF16)


def params(n_axes=0, **kwargs):
    if n_axes:
        kwargs["dimension_semantics"] = ("arbitrary",) * n_axes
    kwargs.setdefault("vmem_limit_bytes", VMEM_ALL)
    return pltpu.CompilerParams(**kwargs)


def vmem():
    return pl.BlockSpec(memory_space=pltpu.VMEM)


def chunk_bounds(starts, tile_idx, width=1):
    lo, hi = starts[tile_idx * width], starts[(tile_idx + 1) * width]
    first = lo // CHUNK
    return first, jnp.where(hi > lo, (hi + CHUNK - 1) // CHUNK, first)


def lookup_kernel(starts, ids_ref, rank_ref, table_ref, out_ref, acc, packed, total):
    tile_idx = pl.program_id(0)
    n_tiles = pl.num_programs(0)
    @pl.when(tile_idx == 0)
    def _():
        acc[...] = jnp.zeros_like(acc)

    first, last = chunk_bounds(starts, tile_idx, LOOK_STEP // LOOK_TILE)
    base = starts[starts.shape[0] - 1] + tile_idx * LOOK_STEP

    def step(c, _):
        rows = lax.broadcasted_iota(jnp.int32, (LOOK_STEP, CHUNK), 0) + base
        acc[c] += mm(table_ref[...], one_hot(rows == ids_ref[c]))
        return 0

    lax.fori_loop(first, last, step, 0)

    @pl.when(tile_idx == n_tiles - 1)
    def _():
        slot = lax.broadcasted_iota(jnp.int32, (rank_ref.shape[1], CHUNK), 1)
        used_first, used_last = chunk_bounds(starts, 0, starts.shape[0] - 2)

        def pack(c, _):
            packed[c] = acc[c].astype(BF16)
            return 0

        lax.fori_loop(used_first, used_last, pack, 0)

        def back(m, _):
            total[...] = jnp.zeros_like(total)

            def add(c, _):
                total[...] += mm(one_hot(slot + c * CHUNK == rank_ref[m]), packed[c], NT)
                return 0

            lax.fori_loop(used_first, used_last, add, 0)
            out_ref[m] = total[...].astype(BF16)
            return 0

        lax.fori_loop(0, out_ref.shape[0], back, 0)


def run_lookup(starts, ids_rows, rank_cols, table_t):
    dim, rows = table_t.shape
    n_micro, tokens = rank_cols.shape[:2]
    n_chunk = n_micro * tokens // CHUNK
    whole = lambda *shape: pl.BlockSpec(shape, lambda i, s: (0,) * len(shape))
    return pl.pallas_call(
        lookup_kernel,
        out_shape=jax.ShapeDtypeStruct((n_micro, tokens, dim), BF16),
        grid_spec=pltpu.PrefetchScalarGridSpec(
            num_scalar_prefetch=1,
            grid=(rows // LOOK_STEP,),
            in_specs=[whole(n_chunk, 1, CHUNK), whole(n_micro, tokens, 1), pl.BlockSpec((dim, LOOK_STEP), lambda i, s: (0, i))],
            out_specs=whole(n_micro, tokens, dim),
            scratch_shapes=[pltpu.VMEM((n_chunk, dim, CHUNK), F32), pltpu.VMEM((n_chunk, dim, CHUNK), BF16), pltpu.VMEM((tokens, dim), F32)],
        ),
        compiler_params=params(1),
        name="lookup",
    )(starts, ids_rows, rank_cols, table_t)


def peer_copy(src, dst, send, recv, slot, group, stage):
    return pltpu.make_async_remote_copy(
        src_ref=src.at[slot], dst_ref=dst.at[slot], send_sem=send.at[slot], recv_sem=recv.at[slot],
        device_id=(group, stage), device_id_type=MESH)


def greet(group, stage, n_stage):
    barrier = pltpu.get_barrier_semaphore()
    for off in range(1, n_stage):
        pl.semaphore_signal(barrier, inc=1, device_id=(group, lax.rem(stage + off, n_stage)), device_id_type=MESH)
    pl.semaphore_wait(barrier, n_stage - 1)


def each(count, body):
    def step(m, _):
        body(m)
        return 0

    lax.fori_loop(0, count, step, 0)


def gelu_parts(pre):
    square = pre * pre
    th = jnp.tanh(pre * (GELU_A + (GELU_A * GELU_B) * square))
    return th, 0.5 + 0.5 * th, square


def fwd_kernel(scale, part, w1_in, w2_in, labels, table, saved_out, last_out, tile_max, tile_sum, tile_pick, prob_out,
               w1, w2, saved, last, near, far, outbox, acc, normed, rows_buf, prob_buf,
               near_s, near_r, far_s, far_r, act_s, act_r, top_s, top2_s, top_r, saved_sem, last_sem, rows_sem, prob_sem, weight_sem):
    group, stage = lax.axis_index("dp"), lax.axis_index("stage")
    count, micro = part.shape[:2]
    block = HEAD_MICRO * micro
    n_block = count // HEAD_MICRO
    n_tiles = table.shape[1] // HEAD_TILE
    n_sub = HEAD_TILE // HEAD_SUB

    def rows_copy(step):
        return pltpu.make_async_copy(
            table.at[:, pl.ds(pl.multiple_of(lax.rem(step, n_tiles) * HEAD_TILE, HEAD_TILE), HEAD_TILE)],
            rows_buf.at[lax.rem(step, 2)], rows_sem.at[lax.rem(step, 2)])

    def prob_copy(step):
        return pltpu.make_async_copy(
            prob_buf.at[lax.rem(step, 2)],
            prob_out.at[pl.ds(pl.multiple_of(step // n_tiles * block, block), block), pl.ds(pl.multiple_of(lax.rem(step, n_tiles) * HEAD_TILE, HEAD_TILE), HEAD_TILE)],
            prob_sem.at[lax.rem(step, 2)])

    def saved_copy(m):
        return pltpu.make_async_copy(saved.at[m], saved_out.at[m], saved_sem.at[m])

    def last_copy(m):
        return pltpu.make_async_copy(last.at[m], last_out.at[m], last_sem.at[m])

    weight_copies = (pltpu.make_async_copy(w1_in, w1, weight_sem.at[0]), pltpu.make_async_copy(w2_in, w2, weight_sem.at[1]))
    for copy in weight_copies:
        copy.start()
    rows_copy(0).start()
    ffn = w1.shape[1]
    greet(group, stage, 4)

    def near_copy(m):
        return peer_copy(part, near, near_s, near_r, m, group, jnp.maximum(stage - 1, 0))

    def far_copy(m):
        return peer_copy(far, far, far_s, far_r, m, group, 0)

    def act_copy(m):
        return peer_copy(outbox, saved, act_s, act_r, m, group, jnp.minimum(stage + 1, 3))

    def top_copy(m, target, sem):
        return peer_copy(last, last, sem, top_r, m, group, target)

    odd = lax.rem(stage, 2) == 1

    @pl.when(odd)
    def _():
        each(count, lambda m: near_copy(m).start())

    @pl.when(stage == 2)
    def _():
        def body(m):
            near_copy(m).wait_recv()
            far[m] = part[m] + near[m]
            far_copy(m).start()

        each(count, body)

    def layer(m):
        @pl.when(stage == 0)
        def _():
            near_copy(m).wait_recv()
            pltpu.make_async_remote_copy(
                src_ref=far.at[m], dst_ref=far.at[m], send_sem=far_s.at[m], recv_sem=far_r.at[m],
                device_id=(group, 2), device_id_type=MESH).wait_recv()
            saved[m] = part[m] + near[m] + far[m]

        @pl.when(stage > 0)
        def _():
            pltpu.make_async_remote_copy(
                src_ref=outbox.at[m], dst_ref=saved.at[m], send_sem=act_s.at[m], recv_sem=act_r.at[m],
                device_id=(group, jnp.maximum(stage - 1, 0)), device_id_type=MESH).wait_recv()

        acts = saved[m]
        for j in range(ffn // FFN_TILE):
            cols = pl.ds(j * FFN_TILE, FFN_TILE)
            pre = mm(acts, w1[:, cols])
            hidden = (pre * gelu_parts(pre)[1]).astype(BF16)
            prod = mm(hidden, w2[:, cols], NT)
            if j == 0:
                acc[...] = prod
            else:
                acc[...] += prod
        result = (acts.astype(F32) + acc[...]).astype(BF16)
        saved_copy(m).start()

        @pl.when(stage < 3)
        def _():
            outbox[m] = result
            act_copy(m).start()

        @pl.when(stage == 3)
        def _():
            last[m] = result
            top_copy(m, 1, top_s).start()
            top_copy(m, 2, top2_s).start()

    def head_tile(step):
        slot = lax.rem(step, 2)
        rows = pl.ds(pl.multiple_of(step // n_tiles * block, block), block)
        tile_idx = lax.rem(step, n_tiles)

        @pl.when(step + 1 < n_block * n_tiles)
        def _():
            rows_copy(step + 1).start()

        rows_copy(step).wait()

        @pl.when(step >= 2)
        def _():
            prob_copy(step - 2).wait()

        acts = normed[...]
        lane = lax.broadcasted_iota(jnp.int32, (block, 128), 1)
        cols = lax.broadcasted_iota(jnp.int32, (block, HEAD_SUB), 1)
        tops, sums, picks = tile_max[rows, :], tile_sum[rows, :], tile_pick[rows, :]
        for q in range(n_sub):
            sub = pl.ds(q * HEAD_SUB, HEAD_SUB)
            raw = mm(acts, rows_buf[slot, :, sub])
            top = jnp.max(raw, axis=1, keepdims=True)
            prob = jnp.exp2((raw - top) * (scale * LOG2_E))
            prob_buf[slot, :, sub] = prob.astype(BF16)
            match = cols == labels[rows, :] - (tile_idx * HEAD_TILE + q * HEAD_SUB)
            picked = jnp.sum(jnp.where(match, raw, 0.0), axis=1, keepdims=True)
            here = lane == tile_idx * n_sub + q
            tops = jnp.where(here, top * scale, tops)
            sums = jnp.where(here, jnp.sum(prob, axis=1, keepdims=True), sums)
            picks = jnp.where(here, picked * scale, picks)
        tile_max[rows, :], tile_sum[rows, :], tile_pick[rows, :] = tops, sums, picks
        prob_copy(step).start()

    def head_block(b):
        for i in range(HEAD_MICRO):
            m = b * HEAD_MICRO + i

            @pl.when(stage == 1)
            def _():
                top_copy(m, 0, top_s).wait_recv()
                top_copy(m, 0, top_s).start()

            @pl.when(lax.rem(stage, 2) == 0)
            def _():
                top_copy(m, 3, top_s).wait_recv()

            last_copy(m).start()
            acts = last[m].astype(F32)
            inv = lax.rsqrt(jnp.mean(acts * acts, axis=-1, keepdims=True) + NORM_EPS)
            normed[pl.ds(i * micro, micro), :] = (acts * inv).astype(BF16)

        each(n_tiles, lambda j: head_tile(b * n_tiles + j))

    tile_max[...] = jnp.full(tile_max.shape, jnp.finfo(F32).min, F32)
    tile_sum[...] = jnp.zeros(tile_sum.shape, F32)
    tile_pick[...] = jnp.zeros(tile_pick.shape, F32)
    first_head = jnp.where(stage == 3, count // 2, jnp.where(stage == 2, count // 2 + 1, count))

    def work(k):
        head = jnp.logical_or(k == first_head, k > count)

        @pl.when(head)
        def _():
            head_block(jnp.maximum(k - count, 0))

        @pl.when(jnp.logical_not(head))
        def _():
            layer(jnp.where(k < first_head, k, k - 1))

    for copy in weight_copies:
        copy.wait()
    each(count + n_block, work)
    each(count, lambda m: saved_copy(m).wait())
    each(count, lambda m: last_copy(m).wait())
    for step in range(n_block * n_tiles - 2, n_block * n_tiles):
        prob_copy(step).wait()

    @pl.when(stage == 1)
    def _():
        each(count, lambda m: top_copy(m, 0, top_s).wait_send())

    @pl.when(odd)
    def _():
        each(count, lambda m: near_copy(m).wait_send())

    @pl.when(stage == 2)
    def _():
        each(count, lambda m: far_copy(m).wait_send())

    @pl.when(stage < 3)
    def _():
        each(count, lambda m: act_copy(m).wait_send())

    @pl.when(stage == 3)
    def _():
        def body(m):
            top_copy(m, 1, top_s).wait_send()
            top_copy(m, 2, top2_s).wait_send()

        each(count, body)


def run_forward(part, w1, w2, labels, table_t, scale):
    count, micro, dim = part.shape
    shape = part.shape
    rows = table_t.shape[1]
    block = HEAD_MICRO * micro
    any_spec = pl.BlockSpec(memory_space=pl.ANY)
    stat = jax.ShapeDtypeStruct((count * micro, 128), F32)
    return pl.pallas_call(
        functools.partial(fwd_kernel, scale),
        out_shape=(jax.ShapeDtypeStruct(shape, BF16), jax.ShapeDtypeStruct(shape, BF16), stat, stat, stat, jax.ShapeDtypeStruct((count * micro, rows), BF16)),
        in_specs=[vmem(), any_spec, any_spec, vmem(), any_spec],
        out_specs=(any_spec,) * 2 + (vmem(),) * 3 + (any_spec,),
        scratch_shapes=[pltpu.VMEM(w1.shape, BF16)] * 2 + [pltpu.VMEM(shape, BF16)] * 5 + [
            pltpu.VMEM((micro, dim), F32), pltpu.VMEM((block, dim), BF16), pltpu.VMEM((2, dim, HEAD_TILE), BF16), pltpu.VMEM((2, block, HEAD_TILE), BF16),
        ] + [pltpu.SemaphoreType.DMA((count,))] * 11 + [pltpu.SemaphoreType.DMA((2,))] * 3,
        compiler_params=params(collective_id=0, has_side_effects=True),
        name="forward",
    )(part, w1, w2, labels, table_t)


def head_grad_kernel(prob_ref, coef_ref, lab_ref, lab_coef_ref, table_ref, grad_ref, out_ref, acc):
    tile_idx = pl.program_id(1)
    n_sub = GRAD_TILE // HEAD_SUB

    @pl.when(tile_idx == 0)
    def _():
        acc[...] = jnp.zeros_like(acc)

    cols = lax.broadcasted_iota(jnp.int32, (GRAD_SUB, HEAD_SUB), 1)
    for r in range(GRAD_ROWS // GRAD_SUB):
        rows = pl.ds(r * GRAD_SUB, GRAD_SUB)
        coefs = pltpu.roll(coef_ref[rows, :], lax.rem(128 - tile_idx * n_sub, 128), 1)
        pieces = []
        for q in range(n_sub):
            sub = pl.ds(q * HEAD_SUB, HEAD_SUB)
            match = cols == lab_ref[rows, :] - (tile_idx * GRAD_TILE + q * HEAD_SUB)
            grad = jnp.where(match, lab_coef_ref[rows, :], prob_ref[rows, sub].astype(F32) * coefs[:, q:q + 1]).astype(BF16)
            grad_ref[rows, sub] = grad
            pieces.append(grad)
        acc[rows, :] += mm(jnp.concatenate(pieces, axis=1), table_ref[...], NT)

    @pl.when(tile_idx == pl.num_programs(1) - 1)
    def _():
        out_ref[...] = acc[...]


def run_head_grad(prob, coef, labels, lab_coef, table_t):
    tokens, rows = prob.shape
    dim = table_t.shape[0]
    tile = pl.BlockSpec((GRAD_ROWS, GRAD_TILE), lambda i, j: (i, j))
    col = pl.BlockSpec((GRAD_ROWS, 1), lambda i, j: (i, 0))
    return pl.pallas_call(
        head_grad_kernel,
        out_shape=(jax.ShapeDtypeStruct((tokens, rows), BF16), jax.ShapeDtypeStruct((tokens, dim), F32)),
        grid=(tokens // GRAD_ROWS, rows // GRAD_TILE),
        in_specs=[tile, pl.BlockSpec((GRAD_ROWS, 128), lambda i, j: (i, 0)), col, col, pl.BlockSpec((dim, GRAD_TILE), lambda i, j: (0, j))],
        out_specs=(tile, pl.BlockSpec((GRAD_ROWS, dim), lambda i, j: (i, 0))),
        scratch_shapes=[pltpu.VMEM((GRAD_ROWS, dim), F32)],
        compiler_params=params(2),
        name="head_grad",
    )(prob, coef, labels, lab_coef, table_t)


def bwd_kernel(gn, last, saved, w1_in, w2_in, gx, first_out, second_out,
               w1, w2, first, second, near, far, dy, outbox, own, top, acts_buf, hid, dpre, acc,
               near_s, near_r, far_s, far_r, act_s, act_r, low_s, low2_s, low_r, own_sem, top_sem, acts_sem, weight_sem, first_sem, second_sem):
    group, stage = lax.axis_index("dp"), lax.axis_index("stage")
    count = near.shape[0]
    ffn = w1.shape[1]
    even = lax.rem(stage, 2) == 0

    def local_copy(src, dst, sem, m):
        return pltpu.make_async_copy(src.at[m], dst.at[lax.rem(m, 2)], sem.at[lax.rem(m, 2)])

    def near_copy(m):
        return peer_copy(gn, near, near_s, near_r, m, group, jnp.where(even, stage + 1, stage - 1))

    def far_copy(m, target):
        return peer_copy(far, far, far_s, far_r, m, group, target)

    def act_copy(m, target):
        return pltpu.make_async_remote_copy(
            src_ref=outbox.at[lax.rem(m, 2)], dst_ref=dy.at[m], send_sem=act_s.at[m], recv_sem=act_r.at[m],
            device_id=(group, target), device_id_type=MESH)

    def low_copy(m, target, sem):
        return peer_copy(gx, gx, sem, low_r, m, group, target)

    def own_copy(m):
        return local_copy(gn, own, own_sem, m)

    def top_copy(m):
        return local_copy(last, top, top_sem, m)

    def acts_copy(m):
        return local_copy(saved, acts_buf, acts_sem, m)

    def tile_copy(src, dst, sem, j):
        cols = pl.ds(j * FFN_TILE, FFN_TILE)
        return pltpu.make_async_copy(src.at[:, cols], dst.at[:, cols], sem.at[j])

    weight_copies = (pltpu.make_async_copy(w1_in, w1, weight_sem.at[0]), pltpu.make_async_copy(w2_in, w2, weight_sem.at[1]))
    for copy in weight_copies:
        copy.start()
    acts_copy(0).start()

    @pl.when(stage == 3)
    def _():
        top_copy(0).start()

    @pl.when(jnp.logical_not(even))
    def _():
        own_copy(0).start()

    greet(group, stage, 4)

    @pl.when(even)
    def _():
        each(count, lambda m: near_copy(m).start())

    first[...] = jnp.zeros_like(first)
    second[...] = jnp.zeros_like(second)

    def advance(copy, m):
        @pl.when(m + 1 < count)
        def _():
            copy(m + 1).start()

        copy(m).wait()

    @pl.when(stage == 1)
    def _():
        def body(m):
            advance(own_copy, m)
            near_copy(m).wait_recv()
            far[m] = (own[lax.rem(m, 2)] + near[m]).astype(BF16)
            far_copy(m, 3).start()

        each(count, body)

    def layer(m):
        slot = lax.rem(m, 2)
        advance(acts_copy, m)

        @pl.when(stage == 3)
        def _():
            advance(own_copy, m)
            advance(top_copy, m)
            near_copy(m).wait_recv()
            far_copy(m, 1).wait_recv()
            grad_n = own[slot] + near[m] + far[m].astype(F32)
            acts = top[slot].astype(F32)
            inv = lax.rsqrt(jnp.mean(acts * acts, axis=-1, keepdims=True) + NORM_EPS)
            inner = jnp.mean(acts * grad_n, axis=-1, keepdims=True)
            dy[m] = (inv * (grad_n - acts * (inv * inv * inner))).astype(BF16)

        @pl.when(stage < 3)
        def _():
            act_copy(m, jnp.minimum(stage + 1, 3)).wait_recv()

        acts = acts_buf[slot]
        grad = dy[m]
        for j in range(ffn // FFN_TILE):
            cols = pl.ds(j * FFN_TILE, FFN_TILE)
            pre = mm(acts, w1[:, cols])
            th, half, square = gelu_parts(pre)
            value = pre * half
            hid[:, cols] = value.astype(BF16)
            slope = half + value * (1.0 - th) * (GELU_A + (3.0 * GELU_A * GELU_B) * square)
            down = (mm(grad, w2[:, cols]) * slope).astype(BF16)
            dpre[:, cols] = down
            prod = mm(down, w1[:, cols], NT)
            if j == 0:
                acc[...] = prod
            else:
                acc[...] += prod
        result = (grad.astype(F32) + acc[...]).astype(BF16)

        @pl.when(stage > 0)
        def _():
            @pl.when(m >= 2)
            def _():
                act_copy(m - 2, jnp.maximum(stage - 1, 0)).wait_send()

            outbox[slot] = result
            act_copy(m, jnp.maximum(stage - 1, 0)).start()

        @pl.when(stage == 0)
        def _():
            gx[m] = result
            low_copy(m, 1, low_s).start()
            low_copy(m, 2, low2_s).start()

        acts_t, grad_t = acts.T, grad.T
        for j in range(ffn // FFN_TILE):
            cols = pl.ds(j * FFN_TILE, FFN_TILE)
            first[:, cols] += mm(acts_t, dpre[:, cols])
            second[:, cols] += mm(grad_t, hid[:, cols])

            @pl.when(m == count - 1)
            def _():
                tile_copy(first, first_out, first_sem, j).start()
                tile_copy(second, second_out, second_sem, j).start()

    for copy in weight_copies:
        copy.wait()
    each(count, layer)

    @pl.when(stage == 2)
    def _():
        def body(m):
            low_copy(m, 3, low_s).wait_recv()
            low_copy(m, 3, low_s).start()

        each(count, body)
        each(count, lambda m: low_copy(m, 3, low_s).wait_send())

    @pl.when(jnp.logical_not(even))
    def _():
        each(count, lambda m: low_copy(m, 0, low_s).wait_recv())

    @pl.when(even)
    def _():
        each(count, lambda m: near_copy(m).wait_send())

    @pl.when(stage == 1)
    def _():
        each(count, lambda m: far_copy(m, 3).wait_send())

    @pl.when(stage > 0)
    def _():
        for m in range(count - 2, count):
            act_copy(m, jnp.maximum(stage - 1, 0)).wait_send()

    @pl.when(stage == 0)
    def _():
        def body(m):
            low_copy(m, 1, low_s).wait_send()
            low_copy(m, 2, low2_s).wait_send()

        each(count, body)

    for j in range(ffn // FFN_TILE):
        tile_copy(first, first_out, first_sem, j).wait()
        tile_copy(second, second_out, second_sem, j).wait()


def run_backward(gn, last, saved, w1, w2):
    shape = saved.shape
    count, tokens, dim = shape
    ffn = w1.shape[1]
    any_spec = pl.BlockSpec(memory_space=pl.ANY)
    pair = lambda dtype: pltpu.VMEM((2, tokens, dim), dtype)
    return pl.pallas_call(
        bwd_kernel,
        out_shape=(jax.ShapeDtypeStruct(shape, BF16), jax.ShapeDtypeStruct((dim, ffn), F32), jax.ShapeDtypeStruct((dim, ffn), F32)),
        in_specs=[any_spec] * 5,
        out_specs=(vmem(), any_spec, any_spec),
        scratch_shapes=[pltpu.VMEM((dim, ffn), BF16)] * 2 + [pltpu.VMEM((dim, ffn), F32)] * 2 + [
            pltpu.VMEM(shape, F32), pltpu.VMEM(shape, BF16), pltpu.VMEM(shape, BF16), pair(BF16), pair(F32), pair(BF16), pair(BF16),
            pltpu.VMEM((tokens, ffn), BF16), pltpu.VMEM((tokens, ffn), BF16), pltpu.VMEM((tokens, dim), F32),
        ] + [pltpu.SemaphoreType.DMA((count,))] * 9 + [pltpu.SemaphoreType.DMA((2,))] * 4 + [pltpu.SemaphoreType.DMA((ffn // FFN_TILE,))] * 2,
        compiler_params=params(collective_id=1, has_side_effects=True),
        name="backward",
    )(gn, last, saved, w1, w2)


def table_kernel(starts, ids_ref, rank_ref, last_ref, gx_ref, grad_ref, first_ref, second_ref, out_ref, first_out, second_out, normt, packed):
    tile_idx = pl.program_id(0)
    n_chunk = packed.shape[0]
    n_micro = gx_ref.shape[0]

    @pl.when(tile_idx == 0)
    def _():
        for m in range(n_micro):
            acts = last_ref[m].astype(F32)
            inv = lax.rsqrt(jnp.mean(acts * acts, axis=-1, keepdims=True) + NORM_EPS)
            normt[:, m * acts.shape[0]:(m + 1) * acts.shape[0]] = (acts * inv).astype(BF16).T

        slot = lax.broadcasted_iota(jnp.int32, (rank_ref.shape[1], CHUNK), 1)

        packed[...] = jnp.zeros_like(packed)

        def gather(c, _):
            total = mm(gx_ref[0], one_hot(slot + c * CHUNK == rank_ref[0]), TN)
            for m in range(1, n_micro):
                total += mm(gx_ref[m], one_hot(slot + c * CHUNK == rank_ref[m]), TN)
            packed[c] = total.astype(BF16)
            return 0

        used_first, used_last = chunk_bounds(starts, 0, starts.shape[0] - 2)
        lax.fori_loop(used_first, used_last, gather, 0)

    first, last = chunk_bounds(starts, tile_idx, OUT_TILE // LOOK_TILE)
    base = starts[starts.shape[0] - 1] + tile_idx * OUT_TILE
    rows = lax.broadcasted_iota(jnp.int32, (CHUNK, OUT_TILE), 1) + base
    near = jnp.minimum(first, n_chunk - 1)
    out_ref[...] = mm(normt[...], grad_ref[...]) + mm(packed[near], one_hot(rows == ids_ref[near]))
    first_out[...] = first_ref[...]
    second_out[...] = second_ref[...]

    def step(c, _):
        out_ref[...] += mm(packed[c], one_hot(rows == ids_ref[c]))
        return 0

    lax.fori_loop(first + 1, last, step, 0)


def run_table(starts, ids_cols, rank_cols, last, gx, grad, first, second):
    tokens, rows = grad.shape
    n_micro, micro, dim = gx.shape
    n_chunk = tokens // CHUNK
    steps = rows // OUT_TILE
    width = PASS_TILE
    passed = pl.BlockSpec((dim, width), lambda i, s: (0, jnp.minimum(i, first.shape[1] // width - 1)))
    whole = lambda *shape: pl.BlockSpec(shape, lambda i, s: (0,) * len(shape))
    return pl.pallas_call(
        table_kernel,
        out_shape=(jax.ShapeDtypeStruct((dim, rows), F32),) + (jax.ShapeDtypeStruct(first.shape, F32),) * 2,
        grid_spec=pltpu.PrefetchScalarGridSpec(
            num_scalar_prefetch=1,
            grid=(steps,),
            in_specs=[whole(n_chunk, CHUNK, 1), whole(n_micro, micro, 1), whole(n_micro, micro, dim), whole(n_micro, micro, dim), pl.BlockSpec((tokens, OUT_TILE), lambda i, s: (0, i)), passed, passed],
            out_specs=(pl.BlockSpec((dim, OUT_TILE), lambda i, s: (0, i)), passed, passed),
            scratch_shapes=[pltpu.VMEM((dim, tokens), BF16), pltpu.VMEM((n_chunk, dim, CHUNK), BF16)],
        ),
        compiler_params=params(1),
        name="table",
    )(starts, ids_cols, rank_cols, last, gx, grad, first, second)


def solution(mesh):
    def body(token_ids, label_ids, emb_rows, w_in, w_out):
        stage = lax.axis_index("stage")
        n_micro, micro = token_ids.shape
        rows, dim = emb_rows.shape
        tokens = n_micro * micro
        scale = dim ** -0.5
        row_start = stage * rows
        table_t = emb_rows.T
        w1 = w_in[0]
        w2 = w_out[0].T

        flat = token_ids.reshape(-1)
        order_key = flat * tokens + jnp.arange(tokens, dtype=jnp.int32)
        rank = jnp.sum((order_key[None, :] < order_key[:, None]).astype(jnp.int32), axis=1)
        slots = jnp.arange(tokens, dtype=jnp.int32)
        sorted_ids = jnp.sum(jnp.where(rank[None, :] == slots[:, None], flat[None, :], 0), axis=1)
        edges = row_start + jnp.arange(rows // LOOK_TILE + 1, dtype=jnp.int32) * LOOK_TILE
        starts = jnp.sum((flat[None, :] < edges[:, None]).astype(jnp.int32), axis=1)
        starts = jnp.concatenate([starts, row_start[None]]).astype(jnp.int32)
        rank_cols = rank.reshape(n_micro, micro, 1)
        ids_rows = sorted_ids.reshape(-1, 1, CHUNK)
        ids_cols = sorted_ids.reshape(-1, CHUNK, 1)

        part = run_lookup(starts, ids_rows, rank_cols, table_t)
        labels = (label_ids - row_start).reshape(tokens, 1)
        saved, last, tile_max, tile_sum, tile_pick, prob = run_forward(part, w1, w2, labels, table_t, scale)
        top = jnp.max(tile_max, axis=1)
        total = jnp.sum(tile_sum * jnp.exp(tile_max - top[:, None]), axis=1)
        stats = lax.all_gather(jnp.stack([top, total, jnp.sum(tile_pick, axis=1)]), "stage")
        row_max = jnp.max(stats[:, 0], axis=0)
        row_sum = jnp.sum(stats[:, 1] * jnp.exp(stats[:, 0] - row_max), axis=0)
        picked = jnp.sum(stats[:, 2], axis=0)
        loss = jnp.sum(jnp.log(row_sum) + row_max - picked) / tokens
        coef = jnp.exp(tile_max - row_max[:, None]) / row_sum[:, None] * scale
        lab_coef = (jnp.exp(picked - row_max) / row_sum - 1.0) * scale
        grad, grad_n = run_head_grad(prob, coef, labels, lab_coef[:, None], table_t)

        gx, grad_first, grad_second = run_backward(grad_n.reshape(n_micro, micro, dim), last, saved, w1, w2)
        grad_table, grad_first, grad_second = run_table(starts, ids_cols, rank_cols, last, gx, grad, grad_first, grad_second)
        return loss.reshape(1), grad_first[None], grad_second.T[None], grad_table.T

    return jax.shard_map(
        body,
        mesh=mesh,
        in_specs=(P("dp", None), P("dp", None), P("stage", None), P("stage", None, None), P("stage", None, None)),
        out_specs=(P("dp"), P(("dp", "stage"), None, None), P(("dp", "stage"), None, None), P(("dp", "stage"), None)),
        check_vma=False,
    )
```

```python
import functools

import jax
import jax.numpy as jnp
from jax import lax
from jax.experimental import pallas as pl
from jax.experimental.pallas import tpu as pltpu
from jax.sharding import PartitionSpec as P

NORM_EPS = 1e-6
GELU_A = 0.7978845608028654
GELU_B = 0.044715
NN = (((1,), (0,)), ((), ()))
NT = (((1,), (1,)), ((), ()))
TN = (((0,), (0,)), ((), ()))
MESH = pl.DeviceIdType.MESH
BF16 = jnp.bfloat16
F32 = jnp.float32
VMEM_ALL = 66_000_000
CHUNK = 256
LOOK_TILE = 512
LOOK_STEP = 2048
OUT_TILE = 1024
PASS_TILE = 256
HEAD_MICRO = 2
HEAD_TILE = 3072
HEAD_SUB = 256
GRAD_ROWS = 1024
GRAD_SUB = 512
GRAD_TILE = 2048
LOG2_E = 1.4426950408889634
FFN_TILE = 512


def mm(lhs, rhs, dims=NN):
    return lax.dot_general(lhs, rhs, dims, preferred_element_type=F32)


def one_hot(match):
    return jnp.where(match, 1.0, 0.0).astype(BF16)


def params(n_axes=0, **kwargs):
    if n_axes:
        kwargs["dimension_semantics"] = ("arbitrary",) * n_axes
    kwargs.setdefault("vmem_limit_bytes", VMEM_ALL)
    return pltpu.CompilerParams(**kwargs)


def vmem():
    return pl.BlockSpec(memory_space=pltpu.VMEM)


def chunk_bounds(starts, tile_idx, width=1):
    lo, hi = starts[tile_idx * width], starts[(tile_idx + 1) * width]
    first = lo // CHUNK
    return first, jnp.where(hi > lo, (hi + CHUNK - 1) // CHUNK, first)


def lookup_kernel(starts, ids_ref, rank_ref, table_ref, out_ref, acc, packed, total):
    tile_idx = pl.program_id(0)
    n_tiles = pl.num_programs(0)
    @pl.when(tile_idx == 0)
    def _():
        acc[...] = jnp.zeros_like(acc)

    first, last = chunk_bounds(starts, tile_idx, LOOK_STEP // LOOK_TILE)
    base = starts[starts.shape[0] - 1] + tile_idx * LOOK_STEP

    def step(c, _):
        rows = lax.broadcasted_iota(jnp.int32, (LOOK_STEP, CHUNK), 0) + base
        acc[c] += mm(table_ref[...], one_hot(rows == ids_ref[c]))
        return 0

    lax.fori_loop(first, last, step, 0)

    @pl.when(tile_idx == n_tiles - 1)
    def _():
        slot = lax.broadcasted_iota(jnp.int32, (rank_ref.shape[1], CHUNK), 1)
        used_first, used_last = chunk_bounds(starts, 0, starts.shape[0] - 2)

        def pack(c, _):
            packed[c] = acc[c].astype(BF16)
            return 0

        lax.fori_loop(used_first, used_last, pack, 0)

        def back(m, _):
            total[...] = jnp.zeros_like(total)

            def add(c, _):
                total[...] += mm(one_hot(slot + c * CHUNK == rank_ref[m]), packed[c], NT)
                return 0

            lax.fori_loop(used_first, used_last, add, 0)
            out_ref[m] = total[...].astype(BF16)
            return 0

        lax.fori_loop(0, out_ref.shape[0], back, 0)


def run_lookup(starts, ids_rows, rank_cols, table_t):
    dim, rows = table_t.shape
    n_micro, tokens = rank_cols.shape[:2]
    n_chunk = n_micro * tokens // CHUNK
    whole = lambda *shape: pl.BlockSpec(shape, lambda i, s: (0,) * len(shape))
    return pl.pallas_call(
        lookup_kernel,
        out_shape=jax.ShapeDtypeStruct((n_micro, tokens, dim), BF16),
        grid_spec=pltpu.PrefetchScalarGridSpec(
            num_scalar_prefetch=1,
            grid=(rows // LOOK_STEP,),
            in_specs=[whole(n_chunk, 1, CHUNK), whole(n_micro, tokens, 1), pl.BlockSpec((dim, LOOK_STEP), lambda i, s: (0, i))],
            out_specs=whole(n_micro, tokens, dim),
            scratch_shapes=[pltpu.VMEM((n_chunk, dim, CHUNK), F32), pltpu.VMEM((n_chunk, dim, CHUNK), BF16), pltpu.VMEM((tokens, dim), F32)],
        ),
        compiler_params=params(1),
        name="lookup",
    )(starts, ids_rows, rank_cols, table_t)


def peer_copy(src, dst, send, recv, slot, group, stage):
    return pltpu.make_async_remote_copy(
        src_ref=src.at[slot], dst_ref=dst.at[slot], send_sem=send.at[slot], recv_sem=recv.at[slot],
        device_id=(group, stage), device_id_type=MESH)


def greet(group, stage, n_stage):
    barrier = pltpu.get_barrier_semaphore()
    for off in range(1, n_stage):
        pl.semaphore_signal(barrier, inc=1, device_id=(group, lax.rem(stage + off, n_stage)), device_id_type=MESH)
    pl.semaphore_wait(barrier, n_stage - 1)


def each(count, body):
    def step(m, _):
        body(m)
        return 0

    lax.fori_loop(0, count, step, 0)


def gelu_parts(pre):
    square = pre * pre
    th = jnp.tanh(pre * (GELU_A + (GELU_A * GELU_B) * square))
    return th, 0.5 + 0.5 * th, square


def fwd_kernel(scale, part, w1_in, w2_in, labels, table, saved_out, last_out, tile_max, totals, prob_out,
               tile_sum, tile_pick, w1, w2, saved, last, near, far, outbox, acc, normed, rows_buf, prob_buf,
               near_s, near_r, far_s, far_r, act_s, act_r, top_s, top2_s, top_r, saved_sem, last_sem, rows_sem, prob_sem, weight_sem):
    group, stage = lax.axis_index("dp"), lax.axis_index("stage")
    count, micro = part.shape[:2]
    block = HEAD_MICRO * micro
    n_block = count // HEAD_MICRO
    n_tiles = table.shape[1] // HEAD_TILE
    n_sub = HEAD_TILE // HEAD_SUB

    def rows_copy(step):
        return pltpu.make_async_copy(
            table.at[:, pl.ds(pl.multiple_of(lax.rem(step, n_tiles) * HEAD_TILE, HEAD_TILE), HEAD_TILE)],
            rows_buf.at[lax.rem(step, 2)], rows_sem.at[lax.rem(step, 2)])

    def prob_copy(step):
        return pltpu.make_async_copy(
            prob_buf.at[lax.rem(step, 2)],
            prob_out.at[pl.ds(pl.multiple_of(step // n_tiles * block, block), block), pl.ds(pl.multiple_of(lax.rem(step, n_tiles) * HEAD_TILE, HEAD_TILE), HEAD_TILE)],
            prob_sem.at[lax.rem(step, 2)])

    def saved_copy(m):
        return pltpu.make_async_copy(saved.at[m], saved_out.at[m], saved_sem.at[m])

    def last_copy(m):
        return pltpu.make_async_copy(last.at[m], last_out.at[m], last_sem.at[m])

    weight_copies = (pltpu.make_async_copy(w1_in, w1, weight_sem.at[0]), pltpu.make_async_copy(w2_in, w2, weight_sem.at[1]))
    for copy in weight_copies:
        copy.start()
    rows_copy(0).start()
    ffn = w1.shape[1]
    greet(group, stage, 4)

    def near_copy(m):
        return peer_copy(part, near, near_s, near_r, m, group, jnp.maximum(stage - 1, 0))

    def far_copy(m):
        return peer_copy(far, far, far_s, far_r, m, group, 0)

    def act_copy(m):
        return peer_copy(outbox, saved, act_s, act_r, m, group, jnp.minimum(stage + 1, 3))

    def top_copy(m, target, sem):
        return peer_copy(last, last, sem, top_r, m, group, target)

    odd = lax.rem(stage, 2) == 1

    @pl.when(odd)
    def _():
        each(count, lambda m: near_copy(m).start())

    @pl.when(stage == 2)
    def _():
        def body(m):
            near_copy(m).wait_recv()
            far[m] = part[m] + near[m]
            far_copy(m).start()

        each(count, body)

    def layer(m):
        @pl.when(stage == 0)
        def _():
            near_copy(m).wait_recv()
            pltpu.make_async_remote_copy(
                src_ref=far.at[m], dst_ref=far.at[m], send_sem=far_s.at[m], recv_sem=far_r.at[m],
                device_id=(group, 2), device_id_type=MESH).wait_recv()
            saved[m] = part[m] + near[m] + far[m]

        @pl.when(stage > 0)
        def _():
            pltpu.make_async_remote_copy(
                src_ref=outbox.at[m], dst_ref=saved.at[m], send_sem=act_s.at[m], recv_sem=act_r.at[m],
                device_id=(group, jnp.maximum(stage - 1, 0)), device_id_type=MESH).wait_recv()

        acts = saved[m]
        for j in range(ffn // FFN_TILE):
            cols = pl.ds(j * FFN_TILE, FFN_TILE)
            pre = mm(acts, w1[:, cols])
            hidden = (pre * gelu_parts(pre)[1]).astype(BF16)
            prod = mm(hidden, w2[:, cols], NT)
            if j == 0:
                acc[...] = prod
            else:
                acc[...] += prod
        result = (acts.astype(F32) + acc[...]).astype(BF16)
        saved_copy(m).start()

        @pl.when(stage < 3)
        def _():
            outbox[m] = result
            act_copy(m).start()

        @pl.when(stage == 3)
        def _():
            last[m] = result
            top_copy(m, 1, top_s).start()
            top_copy(m, 2, top2_s).start()

    def head_tile(step):
        slot = lax.rem(step, 2)
        rows = pl.ds(pl.multiple_of(step // n_tiles * block, block), block)
        tile_idx = lax.rem(step, n_tiles)

        @pl.when(step + 1 < n_block * n_tiles)
        def _():
            rows_copy(step + 1).start()

        rows_copy(step).wait()

        @pl.when(step >= 2)
        def _():
            prob_copy(step - 2).wait()

        acts = normed[...]
        lane = lax.broadcasted_iota(jnp.int32, (block, 128), 1)
        cols = lax.broadcasted_iota(jnp.int32, (block, HEAD_SUB), 1)
        tops, sums, picks = tile_max[rows, :], tile_sum[rows, :], tile_pick[rows, :]
        for q in range(n_sub):
            sub = pl.ds(q * HEAD_SUB, HEAD_SUB)
            raw = mm(acts, rows_buf[slot, :, sub])
            top = jnp.max(raw, axis=1, keepdims=True)
            prob = jnp.exp2((raw - top) * (scale * LOG2_E))
            prob_buf[slot, :, sub] = prob.astype(BF16)
            match = cols == labels[rows, :] - (tile_idx * HEAD_TILE + q * HEAD_SUB)
            picked = jnp.sum(jnp.where(match, raw, 0.0), axis=1, keepdims=True)
            here = lane == tile_idx * n_sub + q
            tops = jnp.where(here, top * scale, tops)
            sums = jnp.where(here, jnp.sum(prob, axis=1, keepdims=True), sums)
            picks = jnp.where(here, picked * scale, picks)
        tile_max[rows, :], tile_sum[rows, :], tile_pick[rows, :] = tops, sums, picks
        prob_copy(step).start()

    def head_block(b):
        for i in range(HEAD_MICRO):
            m = b * HEAD_MICRO + i

            @pl.when(stage == 1)
            def _():
                top_copy(m, 0, top_s).wait_recv()
                top_copy(m, 0, top_s).start()

            @pl.when(lax.rem(stage, 2) == 0)
            def _():
                top_copy(m, 3, top_s).wait_recv()

            last_copy(m).start()
            acts = last[m].astype(F32)
            inv = lax.rsqrt(jnp.mean(acts * acts, axis=-1, keepdims=True) + NORM_EPS)
            normed[pl.ds(i * micro, micro), :] = (acts * inv).astype(BF16)

        each(n_tiles, lambda j: head_tile(b * n_tiles + j))
        rows = pl.ds(pl.multiple_of(b * block, block), block)
        tops = tile_max[rows, :]
        top = jnp.max(tops, axis=1, keepdims=True)
        total = jnp.sum(tile_sum[rows, :] * jnp.exp(tops - top), axis=1, keepdims=True)
        picked = jnp.sum(tile_pick[rows, :], axis=1, keepdims=True)
        lane = lax.broadcasted_iota(jnp.int32, (block, 128), 1)
        totals[rows, :] = jnp.where(lane == 0, top, jnp.where(lane == 1, total, picked))

    tile_max[...] = jnp.full(tile_max.shape, jnp.finfo(F32).min, F32)
    tile_sum[...] = jnp.zeros(tile_sum.shape, F32)
    tile_pick[...] = jnp.zeros(tile_pick.shape, F32)
    first_head = jnp.where(stage == 3, count // 2, jnp.where(stage == 2, count // 2 + 1, count))

    def work(k):
        head = jnp.logical_or(k == first_head, k > count)

        @pl.when(head)
        def _():
            head_block(jnp.maximum(k - count, 0))

        @pl.when(jnp.logical_not(head))
        def _():
            layer(jnp.where(k < first_head, k, k - 1))

    for copy in weight_copies:
        copy.wait()
    each(count + n_block, work)
    each(count, lambda m: saved_copy(m).wait())
    each(count, lambda m: last_copy(m).wait())
    for step in range(n_block * n_tiles - 2, n_block * n_tiles):
        prob_copy(step).wait()

    @pl.when(stage == 1)
    def _():
        each(count, lambda m: top_copy(m, 0, top_s).wait_send())

    @pl.when(odd)
    def _():
        each(count, lambda m: near_copy(m).wait_send())

    @pl.when(stage == 2)
    def _():
        each(count, lambda m: far_copy(m).wait_send())

    @pl.when(stage < 3)
    def _():
        each(count, lambda m: act_copy(m).wait_send())

    @pl.when(stage == 3)
    def _():
        def body(m):
            top_copy(m, 1, top_s).wait_send()
            top_copy(m, 2, top2_s).wait_send()

        each(count, body)


def run_forward(part, w1, w2, labels, table_t, scale):
    count, micro, dim = part.shape
    shape = part.shape
    rows = table_t.shape[1]
    block = HEAD_MICRO * micro
    any_spec = pl.BlockSpec(memory_space=pl.ANY)
    stat = jax.ShapeDtypeStruct((count * micro, 128), F32)
    return pl.pallas_call(
        functools.partial(fwd_kernel, scale),
        out_shape=(jax.ShapeDtypeStruct(shape, BF16), jax.ShapeDtypeStruct(shape, BF16), stat, stat, jax.ShapeDtypeStruct((count * micro, rows), BF16)),
        in_specs=[vmem(), any_spec, any_spec, vmem(), any_spec],
        out_specs=(any_spec,) * 2 + (vmem(),) * 2 + (any_spec,),
        scratch_shapes=[pltpu.VMEM(stat.shape, F32)] * 2 + [pltpu.VMEM(w1.shape, BF16)] * 2 + [pltpu.VMEM(shape, BF16)] * 5 + [
            pltpu.VMEM((micro, dim), F32), pltpu.VMEM((block, dim), BF16), pltpu.VMEM((2, dim, HEAD_TILE), BF16), pltpu.VMEM((2, block, HEAD_TILE), BF16),
        ] + [pltpu.SemaphoreType.DMA((count,))] * 11 + [pltpu.SemaphoreType.DMA((2,))] * 3,
        compiler_params=params(collective_id=0, has_side_effects=True),
        name="forward",
    )(part, w1, w2, labels, table_t)


def head_grad_kernel(prob_ref, coef_ref, lab_ref, lab_coef_ref, table_ref, grad_ref, out_ref, acc):
    tile_idx = pl.program_id(1)
    n_sub = GRAD_TILE // HEAD_SUB

    @pl.when(tile_idx == 0)
    def _():
        acc[...] = jnp.zeros_like(acc)

    cols = lax.broadcasted_iota(jnp.int32, (GRAD_SUB, HEAD_SUB), 1)
    for r in range(GRAD_ROWS // GRAD_SUB):
        rows = pl.ds(r * GRAD_SUB, GRAD_SUB)
        coefs = pltpu.roll(coef_ref[rows, :], lax.rem(128 - tile_idx * n_sub, 128), 1)
        pieces = []
        for q in range(n_sub):
            sub = pl.ds(q * HEAD_SUB, HEAD_SUB)
            match = cols == lab_ref[rows, :] - (tile_idx * GRAD_TILE + q * HEAD_SUB)
            grad = jnp.where(match, lab_coef_ref[rows, :], prob_ref[rows, sub].astype(F32) * coefs[:, q:q + 1]).astype(BF16)
            grad_ref[rows, sub] = grad
            pieces.append(grad)
        acc[rows, :] += mm(jnp.concatenate(pieces, axis=1), table_ref[...], NT)

    @pl.when(tile_idx == pl.num_programs(1) - 1)
    def _():
        out_ref[...] = acc[...]


def run_head_grad(prob, coef, labels, lab_coef, table_t):
    tokens, rows = prob.shape
    dim = table_t.shape[0]
    tile = pl.BlockSpec((GRAD_ROWS, GRAD_TILE), lambda i, j: (i, j))
    col = pl.BlockSpec((GRAD_ROWS, 1), lambda i, j: (i, 0))
    return pl.pallas_call(
        head_grad_kernel,
        out_shape=(jax.ShapeDtypeStruct((tokens, rows), BF16), jax.ShapeDtypeStruct((tokens, dim), F32)),
        grid=(tokens // GRAD_ROWS, rows // GRAD_TILE),
        in_specs=[tile, pl.BlockSpec((GRAD_ROWS, 128), lambda i, j: (i, 0)), col, col, pl.BlockSpec((dim, GRAD_TILE), lambda i, j: (0, j))],
        out_specs=(tile, pl.BlockSpec((GRAD_ROWS, dim), lambda i, j: (i, 0))),
        scratch_shapes=[pltpu.VMEM((GRAD_ROWS, dim), F32)],
        compiler_params=params(2),
        name="head_grad",
    )(prob, coef, labels, lab_coef, table_t)


def bwd_kernel(gn, last, saved, w1_in, w2_in, gx, first_out, second_out,
               w1, w2, first, second, near, far, dy, outbox, own, top, acts_buf, hid, dpre, acc,
               near_s, near_r, far_s, far_r, act_s, act_r, low_s, low2_s, low_r, own_sem, top_sem, acts_sem, weight_sem, first_sem, second_sem):
    group, stage = lax.axis_index("dp"), lax.axis_index("stage")
    count = near.shape[0]
    ffn = w1.shape[1]
    even = lax.rem(stage, 2) == 0

    def local_copy(src, dst, sem, m):
        return pltpu.make_async_copy(src.at[m], dst.at[lax.rem(m, 2)], sem.at[lax.rem(m, 2)])

    def near_copy(m):
        return peer_copy(gn, near, near_s, near_r, m, group, jnp.where(even, stage + 1, stage - 1))

    def far_copy(m, target):
        return peer_copy(far, far, far_s, far_r, m, group, target)

    def act_copy(m, target):
        return pltpu.make_async_remote_copy(
            src_ref=outbox.at[lax.rem(m, 2)], dst_ref=dy.at[m], send_sem=act_s.at[m], recv_sem=act_r.at[m],
            device_id=(group, target), device_id_type=MESH)

    def low_copy(m, target, sem):
        return peer_copy(gx, gx, sem, low_r, m, group, target)

    def own_copy(m):
        return local_copy(gn, own, own_sem, m)

    def top_copy(m):
        return local_copy(last, top, top_sem, m)

    def acts_copy(m):
        return local_copy(saved, acts_buf, acts_sem, m)

    def tile_copy(src, dst, sem, j):
        cols = pl.ds(j * FFN_TILE, FFN_TILE)
        return pltpu.make_async_copy(src.at[:, cols], dst.at[:, cols], sem.at[j])

    weight_copies = (pltpu.make_async_copy(w1_in, w1, weight_sem.at[0]), pltpu.make_async_copy(w2_in, w2, weight_sem.at[1]))
    for copy in weight_copies:
        copy.start()
    acts_copy(0).start()

    @pl.when(stage == 3)
    def _():
        top_copy(0).start()

    @pl.when(jnp.logical_not(even))
    def _():
        own_copy(0).start()

    greet(group, stage, 4)

    @pl.when(even)
    def _():
        each(count, lambda m: near_copy(m).start())

    first[...] = jnp.zeros_like(first)
    second[...] = jnp.zeros_like(second)

    def advance(copy, m):
        @pl.when(m + 1 < count)
        def _():
            copy(m + 1).start()

        copy(m).wait()

    @pl.when(stage == 1)
    def _():
        def body(m):
            advance(own_copy, m)
            near_copy(m).wait_recv()
            far[m] = (own[lax.rem(m, 2)] + near[m]).astype(BF16)
            far_copy(m, 3).start()

        each(count, body)

    def layer(m):
        slot = lax.rem(m, 2)
        advance(acts_copy, m)

        @pl.when(stage == 3)
        def _():
            advance(own_copy, m)
            advance(top_copy, m)
            near_copy(m).wait_recv()
            far_copy(m, 1).wait_recv()
            grad_n = own[slot] + near[m] + far[m].astype(F32)
            acts = top[slot].astype(F32)
            inv = lax.rsqrt(jnp.mean(acts * acts, axis=-1, keepdims=True) + NORM_EPS)
            inner = jnp.mean(acts * grad_n, axis=-1, keepdims=True)
            dy[m] = (inv * (grad_n - acts * (inv * inv * inner))).astype(BF16)

        @pl.when(stage < 3)
        def _():
            act_copy(m, jnp.minimum(stage + 1, 3)).wait_recv()

        acts = acts_buf[slot]
        grad = dy[m]
        for j in range(ffn // FFN_TILE):
            cols = pl.ds(j * FFN_TILE, FFN_TILE)
            pre = mm(acts, w1[:, cols])
            th, half, square = gelu_parts(pre)
            value = pre * half
            hid[:, cols] = value.astype(BF16)
            slope = half + value * (1.0 - th) * (GELU_A + (3.0 * GELU_A * GELU_B) * square)
            down = (mm(grad, w2[:, cols]) * slope).astype(BF16)
            dpre[:, cols] = down
            prod = mm(down, w1[:, cols], NT)
            if j == 0:
                acc[...] = prod
            else:
                acc[...] += prod
        result = (grad.astype(F32) + acc[...]).astype(BF16)

        @pl.when(stage > 0)
        def _():
            @pl.when(m >= 2)
            def _():
                act_copy(m - 2, jnp.maximum(stage - 1, 0)).wait_send()

            outbox[slot] = result
            act_copy(m, jnp.maximum(stage - 1, 0)).start()

        @pl.when(stage == 0)
        def _():
            gx[m] = result
            low_copy(m, 1, low_s).start()
            low_copy(m, 2, low2_s).start()

        acts_t, grad_t = acts.T, grad.T
        for j in range(ffn // FFN_TILE):
            cols = pl.ds(j * FFN_TILE, FFN_TILE)
            first[:, cols] += mm(acts_t, dpre[:, cols])
            second[:, cols] += mm(grad_t, hid[:, cols])

            @pl.when(m == count - 1)
            def _():
                tile_copy(first, first_out, first_sem, j).start()
                tile_copy(second, second_out, second_sem, j).start()

    for copy in weight_copies:
        copy.wait()
    each(count, layer)

    @pl.when(stage == 2)
    def _():
        def body(m):
            low_copy(m, 3, low_s).wait_recv()
            low_copy(m, 3, low_s).start()

        each(count, body)
        each(count, lambda m: low_copy(m, 3, low_s).wait_send())

    @pl.when(jnp.logical_not(even))
    def _():
        each(count, lambda m: low_copy(m, 0, low_s).wait_recv())

    @pl.when(even)
    def _():
        each(count, lambda m: near_copy(m).wait_send())

    @pl.when(stage == 1)
    def _():
        each(count, lambda m: far_copy(m, 3).wait_send())

    @pl.when(stage > 0)
    def _():
        for m in range(count - 2, count):
            act_copy(m, jnp.maximum(stage - 1, 0)).wait_send()

    @pl.when(stage == 0)
    def _():
        def body(m):
            low_copy(m, 1, low_s).wait_send()
            low_copy(m, 2, low2_s).wait_send()

        each(count, body)

    for j in range(ffn // FFN_TILE):
        tile_copy(first, first_out, first_sem, j).wait()
        tile_copy(second, second_out, second_sem, j).wait()


def run_backward(gn, last, saved, w1, w2):
    shape = saved.shape
    count, tokens, dim = shape
    ffn = w1.shape[1]
    any_spec = pl.BlockSpec(memory_space=pl.ANY)
    pair = lambda dtype: pltpu.VMEM((2, tokens, dim), dtype)
    return pl.pallas_call(
        bwd_kernel,
        out_shape=(jax.ShapeDtypeStruct(shape, BF16), jax.ShapeDtypeStruct((dim, ffn), F32), jax.ShapeDtypeStruct((dim, ffn), F32)),
        in_specs=[any_spec] * 5,
        out_specs=(vmem(), any_spec, any_spec),
        scratch_shapes=[pltpu.VMEM((dim, ffn), BF16)] * 2 + [pltpu.VMEM((dim, ffn), F32)] * 2 + [
            pltpu.VMEM(shape, F32), pltpu.VMEM(shape, BF16), pltpu.VMEM(shape, BF16), pair(BF16), pair(F32), pair(BF16), pair(BF16),
            pltpu.VMEM((tokens, ffn), BF16), pltpu.VMEM((tokens, ffn), BF16), pltpu.VMEM((tokens, dim), F32),
        ] + [pltpu.SemaphoreType.DMA((count,))] * 9 + [pltpu.SemaphoreType.DMA((2,))] * 4 + [pltpu.SemaphoreType.DMA((ffn // FFN_TILE,))] * 2,
        compiler_params=params(collective_id=1, has_side_effects=True),
        name="backward",
    )(gn, last, saved, w1, w2)


def table_kernel(starts, ids_ref, rank_ref, last_ref, gx_ref, grad_ref, first_ref, second_ref, out_ref, first_out, second_out, normt, packed):
    tile_idx = pl.program_id(0)
    n_chunk = packed.shape[0]
    n_micro = gx_ref.shape[0]

    @pl.when(tile_idx == 0)
    def _():
        for m in range(n_micro):
            acts = last_ref[m].astype(F32)
            inv = lax.rsqrt(jnp.mean(acts * acts, axis=-1, keepdims=True) + NORM_EPS)
            normt[:, m * acts.shape[0]:(m + 1) * acts.shape[0]] = (acts * inv).astype(BF16).T

        slot = lax.broadcasted_iota(jnp.int32, (rank_ref.shape[1], CHUNK), 1)

        packed[...] = jnp.zeros_like(packed)

        def gather(c, _):
            total = mm(gx_ref[0], one_hot(slot + c * CHUNK == rank_ref[0]), TN)
            for m in range(1, n_micro):
                total += mm(gx_ref[m], one_hot(slot + c * CHUNK == rank_ref[m]), TN)
            packed[c] = total.astype(BF16)
            return 0

        used_first, used_last = chunk_bounds(starts, 0, starts.shape[0] - 2)
        lax.fori_loop(used_first, used_last, gather, 0)

    first, last = chunk_bounds(starts, tile_idx, OUT_TILE // LOOK_TILE)
    base = starts[starts.shape[0] - 1] + tile_idx * OUT_TILE
    rows = lax.broadcasted_iota(jnp.int32, (CHUNK, OUT_TILE), 1) + base
    near = jnp.minimum(first, n_chunk - 1)
    out_ref[...] = mm(normt[...], grad_ref[...]) + mm(packed[near], one_hot(rows == ids_ref[near]))
    first_out[...] = first_ref[...]
    second_out[...] = second_ref[...]

    def step(c, _):
        out_ref[...] += mm(packed[c], one_hot(rows == ids_ref[c]))
        return 0

    lax.fori_loop(first + 1, last, step, 0)


def run_table(starts, ids_cols, rank_cols, last, gx, grad, first, second):
    tokens, rows = grad.shape
    n_micro, micro, dim = gx.shape
    n_chunk = tokens // CHUNK
    steps = rows // OUT_TILE
    width = PASS_TILE
    passed = pl.BlockSpec((dim, width), lambda i, s: (0, jnp.minimum(i, first.shape[1] // width - 1)))
    whole = lambda *shape: pl.BlockSpec(shape, lambda i, s: (0,) * len(shape))
    return pl.pallas_call(
        table_kernel,
        out_shape=(jax.ShapeDtypeStruct((dim, rows), F32),) + (jax.ShapeDtypeStruct(first.shape, F32),) * 2,
        grid_spec=pltpu.PrefetchScalarGridSpec(
            num_scalar_prefetch=1,
            grid=(steps,),
            in_specs=[whole(n_chunk, CHUNK, 1), whole(n_micro, micro, 1), whole(n_micro, micro, dim), whole(n_micro, micro, dim), pl.BlockSpec((tokens, OUT_TILE), lambda i, s: (0, i)), passed, passed],
            out_specs=(pl.BlockSpec((dim, OUT_TILE), lambda i, s: (0, i)), passed, passed),
            scratch_shapes=[pltpu.VMEM((dim, tokens), BF16), pltpu.VMEM((n_chunk, dim, CHUNK), BF16)],
        ),
        compiler_params=params(1),
        name="table",
    )(starts, ids_cols, rank_cols, last, gx, grad, first, second)


def solution(mesh):
    def body(token_ids, label_ids, emb_rows, w_in, w_out):
        stage = lax.axis_index("stage")
        n_micro, micro = token_ids.shape
        rows, dim = emb_rows.shape
        tokens = n_micro * micro
        scale = dim ** -0.5
        row_start = stage * rows
        table_t = emb_rows.T
        w1 = w_in[0]
        w2 = w_out[0].T

        flat = token_ids.reshape(-1)
        order_key = flat * tokens + jnp.arange(tokens, dtype=jnp.int32)
        rank = jnp.sum((order_key[None, :] < order_key[:, None]).astype(jnp.int32), axis=1)
        slots = jnp.arange(tokens, dtype=jnp.int32)
        sorted_ids = jnp.sum(jnp.where(rank[None, :] == slots[:, None], flat[None, :], 0), axis=1)
        edges = row_start + jnp.arange(rows // LOOK_TILE + 1, dtype=jnp.int32) * LOOK_TILE
        starts = jnp.sum((flat[None, :] < edges[:, None]).astype(jnp.int32), axis=1)
        starts = jnp.concatenate([starts, row_start[None]]).astype(jnp.int32)
        rank_cols = rank.reshape(n_micro, micro, 1)
        ids_rows = sorted_ids.reshape(-1, 1, CHUNK)
        ids_cols = sorted_ids.reshape(-1, CHUNK, 1)

        part = run_lookup(starts, ids_rows, rank_cols, table_t)
        labels = (label_ids - row_start).reshape(tokens, 1)
        saved, last, tile_max, totals, prob = run_forward(part, w1, w2, labels, table_t, scale)
        stats = lax.all_gather(totals[:, :3].T, "stage")
        row_max = jnp.max(stats[:, 0], axis=0)
        row_sum = jnp.sum(stats[:, 1] * jnp.exp(stats[:, 0] - row_max), axis=0)
        picked = jnp.sum(stats[:, 2], axis=0)
        loss = jnp.sum(jnp.log(row_sum) + row_max - picked) / tokens
        coef = jnp.exp(tile_max - row_max[:, None]) / row_sum[:, None] * scale
        lab_coef = (jnp.exp(picked - row_max) / row_sum - 1.0) * scale
        grad, grad_n = run_head_grad(prob, coef, labels, lab_coef[:, None], table_t)

        gx, grad_first, grad_second = run_backward(grad_n.reshape(n_micro, micro, dim), last, saved, w1, w2)
        grad_table, grad_first, grad_second = run_table(starts, ids_cols, rank_cols, last, gx, grad, grad_first, grad_second)
        return loss.reshape(1), grad_first[None], grad_second.T[None], grad_table.T

    return jax.shard_map(
        body,
        mesh=mesh,
        in_specs=(P("dp", None), P("dp", None), P("stage", None), P("stage", None, None), P("stage", None, None)),
        out_specs=(P("dp"), P(("dp", "stage"), None, None), P(("dp", "stage"), None, None), P(("dp", "stage"), None)),
        check_vma=False,
    )
```
